32 devices in a mesh: blk: 8 (over z, x), span: 4 (over y, core).
Axes of the slice: x: 2, y: 2, z: 4, core: 2. Of those that a mesh axis runs over, the one named last changes fastest.
Arguments:
- fields: float32 [5, 125, 16384], P(None, None, ('blk', 'span')), may hold values from -6 to 6
- section_store: float32 [5, 125, 16384], P(None, None, ('blk', 'span')), may hold values from -6 to 6
- mean_velocity: float32 [3, 125, 16384], P(None, None, ('blk', 'span')), may hold values from -0.6 to 0.6
- sound_speed: float32 [125, 16384], P(None, ('blk', 'span')), may hold values from 0.7 to 1.5
- element_slot: int32 [16384], P(('blk', 'span')), may hold values from 0 to 511, as said below
- face_turn: int32 [8, 16], P('blk', 'span'), may hold values from 0 to 7
- rotor_offset: int32 [16], P('span'), may hold values from 0 to 7
Outputs:
- fields_next: float32 [5, 125, 16384], P(None, None, ('blk', 'span'))
- store_next: float32 [5, 125, 16384], P(None, None, ('blk', 'span'))
The draws below stay inside these ranges and needn't reach their ends.
Inputs may be any that keep to these rules, and one draw needn't show every extreme that they name: `element_slot`: in each aligned block of 512 entries (the elements of one device) every number 0 to 511 appears once.
All inputs are finite; a program needn't handle non-finite values.
Results may differ from the reference program's by a relative error of at most 0.0003.
Values sent between devices are 32-bit elements; how exact they have to be, the bound alone decides.
No kernel may reach another device: no remote copies, remote signals or barrier semaphores. Data moves between devices by JAX's collectives and lax.ppermute only.
A program may use at most 128 MiB of HBM per device.

```python
import jax
import jax.numpy as jnp
import numpy as np
from jax import lax

ORDER = 4
ET = 1
ES = 4
EA = 128
ELEM_DEV = 512
NT = 8
NS = 16
ELEMS = 16384
N_BLK = 8
N_SPAN = 4


def draw_element_slot(key, part):
    block_keys = jax.random.split(jax.random.fold_in(key, 17), ELEMS // ELEM_DEV)

    def block_order(block_key):
        return jax.random.permutation(block_key, ELEM_DEV)
    orders = jax.vmap(block_order)(block_keys)
    return orders.reshape(ELEMS).astype(jnp.int32)


def draw_rotor_offset(key, part):
    row_keys = jax.random.split(jax.random.fold_in(key, 29), 5)
    base = jax.random.randint(row_keys[0], (NS,), 0, NT)
    far_row = N_BLK // 2 * ET + jax.random.randint(row_keys[1], (), 0, ET)
    near_row = jax.random.randint(row_keys[2], (), 1, ET + 1)
    full_row = (N_BLK - 1) * ET + jax.random.randint(row_keys[3], (), 0, ET)
    base = base.at[0].set(far_row).at[1].set(near_row).at[2].set(full_row)
    order = jax.random.permutation(row_keys[4], NS)
    return base[order].astype(jnp.int32)


def touch_ends(drawn, stream_key, low, top_value):
    spot = [jax.random.randint(jax.random.fold_in(stream_key, axis), (), 0, length) for axis, length in enumerate(drawn.shape)]
    main_axis = drawn.shape.index(max(drawn.shape))
    next_to = spot[:main_axis] + [(spot[main_axis] + 1) % drawn.shape[main_axis]] + spot[main_axis + 1:]
    return drawn.at[tuple(spot)].set(low).at[tuple(next_to)].set(top_value)


def shard_levels(key, extent, cuts, least, top_value):
    level, own = 1.0, jax.random.fold_in(key, 6)
    for position, blocks in cuts:
        steps = jnp.exp(jax.random.uniform(jax.random.fold_in(own, position), (blocks,), jnp.float32, least / len(cuts), top_value / len(cuts)))
        level = level * jnp.repeat(steps, extent[position] // blocks).reshape([-1 if axis == position else 1 for axis in range(len(extent))])
    return level


def scatter_about(own_key, dims, spread, most, cuts=(), kind=jnp.bfloat16):
    level = shard_levels(own_key, dims, cuts, -0.22, 0.18) if cuts else 1.0
    drawn = jax.random.normal(own_key, dims, jnp.float32) * spread * level
    return jnp.minimum(jnp.maximum(drawn, -most), most).astype(kind)


def setup_inputs(seed: int = 0) -> dict:
    streams_of = jax.random.split(jax.random.key(seed), 8)
    fields = scatter_about(streams_of[0], (5, (ORDER + 1) ** 3, ELEMS), 1.0, 6.0, ((2, 32),), jnp.float32)
    section_store = scatter_about(streams_of[1], (5, (ORDER + 1) ** 3, ELEMS), 1.0, 6.0, ((2, 32),), jnp.float32)
    mean_velocity = jnp.clip(jax.random.uniform(streams_of[2], (3, (ORDER + 1) ** 3, ELEMS), jnp.float32, -0.6, 0.6) * shard_levels(streams_of[2], (3, (ORDER + 1) ** 3, ELEMS), ((2, 32),), -0.4, 0.0), -0.6, 0.6)
    sound_speed = jnp.clip(0.7 + 0.8 * jax.random.uniform(streams_of[3], ((ORDER + 1) ** 3, ELEMS), jnp.float32) ** shard_levels(streams_of[3], ((ORDER + 1) ** 3, ELEMS), ((1, 32),), -0.2, 0.2), 0.7, 1.5)
    element_slot = draw_element_slot(jax.random.fold_in(streams_of[7], 71), 0)
    face_turn = touch_ends(jax.random.randint(streams_of[5], (NT, NS), 0, 8), jax.random.fold_in(streams_of[5], 1), 0, 7).astype(jnp.int32)
    rotor_offset = draw_rotor_offset(jax.random.fold_in(streams_of[7], 71), 0)
    return dict(fields=fields, section_store=section_store, mean_velocity=mean_velocity, sound_speed=sound_speed, element_slot=element_slot, face_turn=face_turn, rotor_offset=rotor_offset)


section_decay = -567301805773.0 / 1357537059087.0
section_gain = 5161836677717.0 / 13612068292357.0
time_step = 0.05
metric_scale = (1.0, 1.5, 0.75)
end_weight = 0.1

def lobatto_slopes():
    inner_root = np.sqrt(3.0 / 7.0)
    points = np.array([-1.0, -inner_root, 0.0, inner_root, 1.0])
    node_count = points.shape[0]
    slope_values = np.zeros((node_count, node_count))
    for row_index in range(node_count):
        for column_index in range(node_count):
            if row_index == column_index:
                slope_values[row_index, column_index] = sum((1.0 / (points[row_index] - points[other_index]) for other_index in range(node_count) if other_index != row_index))
            else:
                product_row = np.prod([points[row_index] - points[other_index] for other_index in range(node_count) if other_index != row_index])
                product_column = np.prod([points[column_index] - points[other_index] for other_index in range(node_count) if other_index != column_index])
                slope_values[row_index, column_index] = product_row / (product_column * (points[row_index] - points[column_index]))
    return slope_values

def face_of(element_data, direction, which_end):
    return lax.index_in_dim(element_data, which_end, axis=1 + direction, keepdims=False)

def normal_trace(face_data, direction):
    return jnp.concatenate([face_data[:5], face_data[5 + direction:6 + direction], face_data[8:9]], axis=0)

def normal_flux(face_data, direction):
    state_part = face_data[:5]
    flow_speed = face_data[5]
    sound_part = face_data[6]
    normal_velocity = state_part[1 + direction]
    pressure = state_part[4]
    zero_part = jnp.zeros_like(pressure)
    coupled = jnp.stack([normal_velocity] + [pressure if axis_index == direction else zero_part for axis_index in range(3)] + [normal_velocity])
    return flow_speed[None] * state_part + sound_part[None] * coupled

def face_flux(left_side, right_side, direction):
    wave_reach = jnp.maximum(jnp.abs(left_side[5]) + left_side[6], jnp.abs(right_side[5]) + right_side[6])
    return 0.5 * (normal_flux(left_side, direction) + normal_flux(right_side, direction)) - 0.5 * wave_reach[None] * (right_side[:5] - left_side[:5])

def wall_ghost(face_data):
    flip_sign = jnp.array([1.0, 1.0, -1.0, 1.0, 1.0, 1.0, 1.0], jnp.float32).reshape((7,) + (1,) * (face_data.ndim - 1))
    return face_data * flip_sign

def turn_face(face_data, turn_codes, inverse):
    result = jnp.zeros_like(face_data)
    for turn_code in range(8):
        turned = face_data
        if inverse:
            if turn_code & 2:
                turned = jnp.flip(turned, 2)
            if turn_code & 1:
                turned = jnp.flip(turned, 1)
            if turn_code & 4:
                turned = jnp.swapaxes(turned, 1, 2)
        else:
            if turn_code & 4:
                turned = jnp.swapaxes(turned, 1, 2)
            if turn_code & 1:
                turned = jnp.flip(turned, 1)
            if turn_code & 2:
                turned = jnp.flip(turned, 2)
        result = result + jnp.where(turn_codes == turn_code, turned, 0.0)
    return result

def pick_cells(cycle_data, cell_index):
    full_index = jnp.broadcast_to(cell_index[None, None, None], cycle_data.shape[:3] + cell_index.shape)
    return jnp.take_along_axis(cycle_data, full_index, axis=3)

def surface_terms(segment, direction, ghost_low, ghost_high):
    plus_side = normal_trace(face_of(segment, direction, 4), direction)
    minus_side = normal_trace(face_of(segment, direction, 0), direction)
    element_axis = 3 + direction
    left_side = jnp.concatenate([ghost_low, plus_side], axis=element_axis)
    right_side = jnp.concatenate([minus_side, ghost_high], axis=element_axis)
    fluxes = face_flux(left_side, right_side, direction)
    face_total = fluxes.shape[element_axis]
    upper_part = normal_flux(plus_side, direction) - lax.slice_in_dim(fluxes, 1, face_total, axis=element_axis)
    lower_part = lax.slice_in_dim(fluxes, 0, face_total - 1, axis=element_axis) - normal_flux(minus_side, direction)
    mark_shape = [1] * 7
    mark_shape[1 + direction] = 5
    high_mark = (jnp.arange(5) == 4).astype(jnp.float32).reshape(mark_shape)
    low_mark = (jnp.arange(5) == 0).astype(jnp.float32).reshape(mark_shape)
    weight = metric_scale[direction] / end_weight
    return weight * (jnp.expand_dims(upper_part, 1 + direction) * high_mark + jnp.expand_dims(lower_part, 1 + direction) * low_mark)

def volume_terms(element_data):
    slope_table = jnp.asarray(lobatto_slopes(), jnp.float32)
    einsum_forms = ('ni,fijkxyz->fnjkxyz', 'nj,fijkxyz->finkxyz', 'nk,fijkxyz->fijnxyz')
    summed = jnp.zeros((5,) + element_data.shape[1:], jnp.float32)
    for direction in range(3):
        volume_flux = normal_flux(normal_trace(element_data, direction), direction)
        summed = summed - metric_scale[direction] * jnp.einsum(einsum_forms[direction], slope_table, volume_flux, precision=lax.Precision.HIGHEST)
    return summed

def block_rates(element_data, theta_low, theta_high, span_low, span_high, from_rotor, from_stator):
    half_axial = element_data.shape[6] // 2
    rates = volume_terms(element_data)
    rates = rates + surface_terms(element_data, 0, theta_low, theta_high)
    rates = rates + surface_terms(element_data, 1, span_low, span_high)
    stator = element_data[..., :half_axial]
    rotor = element_data[..., half_axial:]
    inlet_trace = normal_trace(face_of(stator, 2, 0)[..., 0:1], 2)
    inlet = jnp.concatenate([jnp.zeros_like(inlet_trace[:5]), inlet_trace[5:]], axis=0)
    outlet_trace = normal_trace(face_of(rotor, 2, 4)[..., half_axial - 1:half_axial], 2)
    outlet = jnp.concatenate([jnp.zeros_like(outlet_trace[:5]), outlet_trace[5:]], axis=0)
    axial_terms = jnp.concatenate([surface_terms(stator, 2, inlet, from_rotor), surface_terms(rotor, 2, from_stator, outlet)], axis=6)
    return rates + axial_terms

def reference(fields, section_store, mean_velocity, sound_speed, element_slot, face_turn, rotor_offset):
    node_count = ORDER + 1
    block_count = N_BLK * N_SPAN
    half_axial = EA // 2
    cycle_size = ET * N_BLK
    block_turns = face_turn.reshape(N_BLK, ET, N_SPAN, ES)

    def block_data(block_index):
        start = block_index * ELEM_DEV
        slots = lax.dynamic_slice_in_dim(element_slot, start, ELEM_DEV, 0)
        local_fields = lax.dynamic_slice_in_dim(fields, start, ELEM_DEV, 2)
        local_velocity = lax.dynamic_slice_in_dim(mean_velocity, start, ELEM_DEV, 2)
        local_sound = lax.dynamic_slice_in_dim(sound_speed, start, ELEM_DEV, 1)
        stacked = jnp.concatenate([local_fields, local_velocity, local_sound[None]], axis=0)
        element_data = jnp.take(stacked, slots, axis=2).reshape(9, node_count, node_count, node_count, ET, ES, EA)
        return (slots, element_data)

    def codes_of(block_index):
        return block_turns[block_index // N_SPAN, :, block_index % N_SPAN, :]

    def trace_pass(block_index):
        slots, element_data = block_data(block_index)
        theta_pair = jnp.concatenate([face_of(element_data, 0, 0)[:, :, :, 0:1], face_of(element_data, 0, 4)[:, :, :, ET - 1:ET]], axis=3)
        span_pair = jnp.concatenate([face_of(element_data, 1, 0)[:, :, :, :, 0:1], face_of(element_data, 1, 4)[:, :, :, :, ES - 1:ES]], axis=4)
        stator_face = face_of(element_data, 2, 4)[..., half_axial - 1]
        rotor_face = turn_face(face_of(element_data, 2, 0)[..., half_axial], codes_of(block_index), True)
        return (theta_pair, span_pair, stator_face, rotor_face)
    block_ids = jnp.arange(block_count, dtype=jnp.int32)
    theta_pairs, span_pairs, stator_faces, rotor_faces = lax.map(trace_pass, block_ids)

    def rate_pass(block_index):
        slots, element_data = block_data(block_index)
        sector = block_index // N_SPAN
        slab_index = block_index % N_SPAN
        before = (sector - 1) % N_BLK * N_SPAN + slab_index
        after = (sector + 1) % N_BLK * N_SPAN + slab_index
        theta_low = normal_trace(theta_pairs[before][:, :, :, 1:2], 0)
        theta_high = normal_trace(theta_pairs[after][:, :, :, 0:1], 0)
        own_span = span_pairs[block_index]
        below = normal_trace(span_pairs[jnp.maximum(block_index - 1, 0)][:, :, :, :, 1:2], 1)
        above = normal_trace(span_pairs[jnp.minimum(block_index + 1, block_count - 1)][:, :, :, :, 0:1], 1)
        hub = wall_ghost(normal_trace(own_span[:, :, :, :, 0:1], 1))
        casing = wall_ghost(normal_trace(own_span[:, :, :, :, 1:2], 1))
        span_low = jnp.where(slab_index > 0, below, hub)
        span_high = jnp.where(slab_index < N_SPAN - 1, above, casing)
        cycle_blocks = jnp.arange(N_BLK, dtype=jnp.int32) * N_SPAN + slab_index
        stator_cycle = jnp.moveaxis(stator_faces[cycle_blocks], 0, 3).reshape(9, node_count, node_count, cycle_size, ES)
        rotor_cycle = jnp.moveaxis(rotor_faces[cycle_blocks], 0, 3).reshape(9, node_count, node_count, cycle_size, ES)
        cycle_cells = sector * ET + jnp.arange(ET, dtype=jnp.int32)
        offsets = lax.dynamic_slice_in_dim(rotor_offset, (slab_index * ES).astype(jnp.int32), ES, 0)
        stator_near = pick_cells(stator_cycle, (cycle_cells[:, None] - offsets[None, :]) % cycle_size)
        rotor_near = pick_cells(rotor_cycle, (cycle_cells[:, None] + offsets[None, :]) % cycle_size)
        from_stator = normal_trace(turn_face(stator_near, codes_of(block_index), False), 2)[..., None]
        from_rotor = normal_trace(rotor_near, 2)[..., None]
        rates = block_rates(element_data, theta_low, theta_high, span_low, span_high, from_rotor, from_stator)
        stored = jnp.zeros((5, node_count ** 3, ELEM_DEV), jnp.float32).at[:, :, slots].set(rates.reshape(5, node_count ** 3, ELEM_DEV))
        start = block_index * ELEM_DEV
        old_store = lax.dynamic_slice_in_dim(section_store, start, ELEM_DEV, 2)
        old_fields = lax.dynamic_slice_in_dim(fields, start, ELEM_DEV, 2)
        new_store = section_decay * old_store + time_step * stored
        new_fields = old_fields + section_gain * new_store
        return (new_fields, new_store)
    fields_blocks, store_blocks = lax.map(rate_pass, block_ids)
    fields_next = jnp.moveaxis(fields_blocks, 0, 2).reshape(5, node_count ** 3, ELEMS)
    store_next = jnp.moveaxis(store_blocks, 0, 2).reshape(5, node_count ** 3, ELEMS)
    return (fields_next, store_next)
```

```python
import functools

import jax
import jax.numpy as jnp
import numpy as np
from jax import lax
from jax.experimental import pallas as pl
from jax.experimental.pallas import tpu as pltpu
from jax.sharding import PartitionSpec as P

ORDER = 4
NODE = ORDER + 1
FACE = NODE * NODE
VOL = NODE**3
LANES = 128
PAD = 32
VALS = 7

section_decay = -567301805773.0 / 1357537059087.0
section_gain = 5161836677717.0 / 13612068292357.0
time_step = 0.05
metric_scale = (1.0, 1.5, 0.75)
end_weight = 0.1

BF = jnp.bfloat16
F32 = jnp.float32
VMEM_LIMIT = 24 * 1024 * 1024


def lobatto_slopes():
    inner_root = np.sqrt(3.0 / 7.0)
    points = np.array([-1.0, -inner_root, 0.0, inner_root, 1.0])
    count = points.shape[0]
    slopes = np.zeros((count, count))
    for r in range(count):
        for c in range(count):
            if r == c:
                slopes[r, c] = sum(1.0 / (points[r] - points[o]) for o in range(count) if o != r)
            else:
                top = np.prod([points[r] - points[o] for o in range(count) if o != r])
                low = np.prod([points[c] - points[o] for o in range(count) if o != c])
                slopes[r, c] = top / (low * (points[r] - points[c]))
    return slopes


def split_np(table):
    high = np.asarray(table, np.float32).astype(BF)
    low = (np.asarray(table, np.float64) - high.astype(np.float64)).astype(BF)
    return high, low


def volume_matrix():
    slopes = lobatto_slopes()
    eye = np.eye(NODE)
    parts = (
        np.kron(np.kron(slopes, eye), eye),
        np.kron(np.kron(eye, slopes), eye),
        np.kron(np.kron(eye, eye), slopes),
    )
    full = np.zeros((LANES, 3 * LANES))
    for d in range(3):
        full[:VOL, d * LANES : d * LANES + VOL] = -time_step * metric_scale[d] * parts[d]
    high, low = split_np(full)
    return np.concatenate([high, low], 0)


def turn_matrix(inverse):
    table = np.zeros((PAD, 8 * PAD), np.float32)
    for code in range(8):
        index = np.arange(FACE).reshape(NODE, NODE)
        if inverse:
            if code & 2:
                index = index[:, ::-1]
            if code & 1:
                index = index[::-1, :]
            if code & 4:
                index = index.T
        else:
            if code & 4:
                index = index.T
            if code & 1:
                index = index[::-1, :]
            if code & 2:
                index = index[:, ::-1]
        for n, o in enumerate(index.reshape(-1)):
            table[n, code * PAD + o] = 1.0
    return table.astype(BF)


def dot(a, b):
    return jnp.dot(a, b, preferred_element_type=F32)


def dot_t(a, b):
    return lax.dot_general(a, b, (((1,), (1,)), ((), ())), preferred_element_type=F32)


def halves(x):
    high = x.astype(BF)
    return high, (x - high.astype(F32)).astype(BF)


def lane_iota(shape):
    return lax.broadcasted_iota(jnp.int32, shape, len(shape) - 1)


def row_iota(shape):
    return lax.broadcasted_iota(jnp.int32, shape, 0)


def face_rows(ref, v, tile, d, end):
    if d == 0:
        return ref[v, tile, pl.ds(end * FACE, FACE), :]
    if d == 1:
        starts = [i * FACE + end * NODE for i in range(NODE)]
        return jnp.concatenate([ref[v, tile, pl.ds(s, NODE), :] for s in starts], axis=0)
    return ref[v, tile, pl.ds(end, FACE, NODE), :]


def add_face_rows(ref, v, tile, d, end, value):
    if d == 0:
        ref[v, tile, pl.ds(end * FACE, FACE), :] += value
    elif d == 1:
        for i in range(NODE):
            ref[v, tile, pl.ds(i * FACE + end * NODE, NODE), :] += value[i * NODE : (i + 1) * NODE]
    else:
        ref[v, tile, pl.ds(end, FACE, NODE), :] += value


def value_index(f, d):
    return f if f < 5 else (5 + d if f == 5 else 8)


def stage_values(fields, velocity, sound, staged, tiles):
    for t in range(tiles):
        cols = slice(t * LANES, (t + 1) * LANES)
        for f in range(5):
            staged[f, t, 0:VOL, :] = fields[f, :, cols]
        for d in range(3):
            staged[5 + d, t, 0:VOL, :] = velocity[d, :, cols]
        staged[8, t, 0:VOL, :] = sound[:, cols]


def surface(own, other, d, side):
    qo, mo, co = own[:5], own[5], own[6]
    qn, mn, cn = other[:5], other[5], other[6]
    reach = jnp.maximum(jnp.abs(mo) + co, jnp.abs(mn) + cn)
    weight = side * 0.5 * time_step * metric_scale[d] / end_weight
    if side > 0:
        ao, an = mo - reach, mn - reach
    else:
        ao, an = mo + reach, mn + reach
    velocity_part = co * qo[1 + d] - cn * qn[1 + d]
    pressure_part = co * qo[4] - cn * qn[4]
    out = []
    for f in range(5):
        x = ao * qo[f] - an * qn[f]
        if f in (0, 4):
            x = x + velocity_part
        elif f == 1 + d:
            x = x + pressure_part
        out.append(weight * x)
    return out


def axis_parity(axis):
    return lax.rem(lax.axis_index(axis), 2)


def pack_kernel(
    per_span, axial, slot_s, turn_s, slot_v, fields, velocity, sound, turn_t,
    th_a, th_b, sp_a, sp_b, iface, staged, rows_hi, rows_lo, stack_hi, stack_lo,
):
    elems = slot_v.shape[1]
    tiles = elems // LANES
    half = axial // 2
    stage_values(fields, velocity, sound, staged, tiles)

    def theta_rows(out, end):
        for f in range(VALS):
            v = value_index(f, 0)
            for t in range(tiles):
                out[f * FACE : (f + 1) * FACE, t * LANES : (t + 1) * LANES] = face_rows(staged, v, t, 0, end * ORDER)
        out[VALS * FACE : VALS * FACE + 1, :] = slot_v[...].astype(F32)

    odd = axis_parity("blk")

    @pl.when(odd == 0)
    def _():
        theta_rows(th_a, 1)
        theta_rows(th_b, 0)

    @pl.when(odd == 1)
    def _():
        theta_rows(th_a, 0)
        theta_rows(th_b, 1)

    def gather_faces(d, end, target):
        for f in range(VALS):
            v = value_index(f, d)
            for t in range(tiles):
                x = face_rows(staged, v, t, d, end * ORDER)
                hi, lo = halves(jnp.concatenate([x, jnp.zeros((PAD - FACE, LANES), F32)], 0))
                rows_hi[f * PAD : (f + 1) * PAD, t * LANES : (t + 1) * LANES] = hi
                rows_lo[f * PAD : (f + 1) * PAD, t * LANES : (t + 1) * LANES] = lo
        one = (row_iota((elems, LANES)) == target).astype(BF)
        return dot(rows_hi[...], one) + dot(rows_lo[...], one)

    low = gather_faces(1, 0, slot_v[:, 0:axial])
    high = gather_faces(1, 1, slot_v[:, elems - axial : elems])
    span_odd = axis_parity("span")

    @pl.when(span_odd == 0)
    def _():
        sp_a[...] = high
        sp_b[...] = low

    @pl.when(span_odd == 1)
    def _():
        sp_a[...] = low
        sp_b[...] = high

    lane = lane_iota((1, LANES))
    column = lane % (2 * per_span)
    target = jnp.full((1, LANES), -1, jnp.int32)
    code = jnp.zeros((1, LANES), jnp.int32)
    for s in range(per_span):
        target = jnp.where(lane == s, slot_s[s * axial + half - 1], target)
        target = jnp.where(lane == per_span + s, slot_s[s * axial + half], target)
        code = jnp.where(column == per_span + s, turn_s[0, s], code)
    stator = gather_faces(2, 1, jnp.where(lane < per_span, target, -1))
    rotor = gather_faces(2, 0, jnp.where(lane < per_span, -1, target))
    both = stator + rotor
    packed = both[0:PAD]
    for f in range(1, VALS):
        packed = packed + pltpu.roll(both[f * PAD : (f + 1) * PAD], f * 2 * per_span, 1)
    iface[...] = turned(packed, code, turn_t, stack_hi, stack_lo)


def turned(packed, code, turn_t, stack_hi, stack_lo):
    hi, lo = packed.astype(BF).astype(F32), None
    lo = packed - hi
    for c in range(8):
        stack_hi[c * PAD : (c + 1) * PAD, :] = jnp.where(code == c, hi, 0.0).astype(BF)
        stack_lo[c * PAD : (c + 1) * PAD, :] = jnp.where(code == c, lo, 0.0).astype(BF)
    return dot(turn_t[...], stack_hi[...]) + dot(turn_t[...], stack_lo[...])


def volume_kernel(fields, velocity, sound, store, matrix, out, flux_hi, flux_lo):
    width = sound.shape[1]
    step = 16
    for r in range(0, VOL, step):
        n = min(step, VOL - r)
        rows = slice(r, r + n)
        q = [fields[f, rows, :] for f in range(5)]
        c = sound[rows, :]
        cp = c * q[4]
        for d in range(3):
            m = velocity[d, rows, :]
            cu = c * q[1 + d]
            for f in range(5):
                x = m * q[f]
                if f in (0, 4):
                    x = x + cu
                elif f == 1 + d:
                    x = x + cp
                if n < step:
                    x = jnp.concatenate([x, jnp.zeros((step - n, width), F32)], 0)
                hi, lo = halves(x)
                flux_hi[f, d * LANES + r : d * LANES + r + step, :] = hi
                flux_lo[f, d * LANES + r : d * LANES + r + step, :] = lo
    for f in range(5):
        a = dot(matrix[...], flux_hi[f])
        b = dot(matrix[0:LANES, :], flux_lo[f])
        total = a[0:LANES] + a[LANES : 2 * LANES] + b
        out[f] = section_decay * store[f] + total[0:VOL]


def neighbour_index(rows, slot_v):
    elems = slot_v.shape[1]
    own = (row_iota((elems, elems)) == slot_v[...]).astype(BF)
    base = 256.0
    table = jnp.concatenate(rows + [jnp.zeros((8 - len(rows), elems), F32)], 0)
    upper = jnp.floor(table * (1.0 / base))
    lower = table - upper * base
    both = jnp.concatenate([upper, lower], 0).astype(BF)
    moved = dot_t(both, own)
    return (moved[0:8] * base + moved[8:16]).astype(jnp.int32)


def pick_matrix(index_row, count):
    return (row_iota((count, index_row.shape[1])) == index_row).astype(BF)


def theta_ghost(recv, slot_v):
    elems = slot_v.shape[1]
    index = neighbour_index([recv[VALS * FACE : VALS * FACE + 1, :]], slot_v)
    one = pick_matrix(index[0:1], elems)
    hi, lo = halves(recv[...])
    return dot(hi, one) + dot(lo, one)


def face_kernel(
    per_span, axial, sectors, slabs, pieces,
    offset_s, turn_s, slot_v, fields, velocity, sound, part, th_a, sp_a, sp_b, turn_t, *rest,
):
    iface = rest[:pieces]
    fields_out, store_out = rest[pieces : pieces + 2]
    staged, acc, rows_hi, rows_lo, stack_hi, stack_lo, ghost = rest[pieces + 2 :]
    elems = slot_v.shape[1]
    tiles = elems // LANES
    half = axial // 2
    stage_values(fields, velocity, sound, staged, tiles)
    for t in range(tiles):
        for f in range(5):
            acc[f, t, 0:VOL, :] = part[f, :, t * LANES : (t + 1) * LANES]

    slots = slot_v[...].astype(F32)
    lane = lane_iota((1, elems))
    position = lane % axial
    row = lane // axial
    lanes_f = lane.astype(F32)
    span_low = jnp.where(lane < axial, elems + lanes_f, pltpu.roll(slots, axial, 1))
    span_high = jnp.where(lane >= elems - axial, axial + lanes_f, pltpu.roll(slots, elems - axial, 1))
    ax_low = jnp.where(position == half, elems + row.astype(F32), pltpu.roll(slots, 1, 1))
    ax_low = jnp.where(position == 0, elems + LANES - 1.0, ax_low)
    ax_high = jnp.where(position == half - 1, elems + per_span + row.astype(F32), pltpu.roll(slots, elems - 1, 1))
    ax_high = jnp.where(position == axial - 1, elems + LANES - 1.0, ax_high)
    index = neighbour_index([span_low, span_high, ax_low, ax_high], slot_v)

    def fill_rows(d, end):
        for f in range(VALS):
            v = value_index(f, d)
            for t in range(tiles):
                x = face_rows(staged, v, t, d, end * ORDER)
                hi, lo = halves(jnp.concatenate([x, jnp.zeros((PAD - FACE, LANES), F32)], 0))
                rows_hi[f * PAD : (f + 1) * PAD, t * LANES : (t + 1) * LANES] = hi
                rows_lo[f * PAD : (f + 1) * PAD, t * LANES : (t + 1) * LANES] = lo

    def one_side(d, side, index_row, extra, wall):
        end = ORDER if side > 0 else 0
        fill_rows(d, 0 if side > 0 else 1)
        hi, lo = halves(extra)
        rows_hi[:, elems : elems + LANES] = hi
        rows_lo[:, elems : elems + LANES] = lo
        one = pick_matrix(index_row, elems + LANES)
        ghost[...] = dot(rows_hi[...], one) + dot(rows_lo[...], one)
        for t in range(tiles):
            cols = slice(t * LANES, (t + 1) * LANES)
            own = [face_rows(staged, value_index(f, d), t, d, end) for f in range(VALS)]
            other = [ghost[f * PAD : f * PAD + FACE, cols] for f in range(VALS)]
            if wall is not None:
                at_wall = jnp.logical_and(index_row[:, cols] >= elems, wall)
                for f in range(VALS):
                    other[f] = jnp.where(at_wall, -own[f] if f == 1 + d else own[f], other[f])
            for f, x in enumerate(surface(own, other, d, side)):
                add_face_rows(acc, f, t, d, end, x)

    slab = lax.axis_index("span")
    slab_odd = lax.rem(slab, 2) == 1
    one_side(1, -1, index[0:1], jnp.where(slab_odd, sp_a[...], sp_b[...]), slab == 0)
    one_side(1, 1, index[1:2], jnp.where(slab_odd, sp_b[...], sp_a[...]), slab == slabs - 1)

    sector = lax.axis_index("blk")
    small = lane_iota((1, LANES))
    column = small % (2 * per_span)
    want = jnp.zeros((1, LANES), jnp.int32)
    code = jnp.zeros((1, LANES), jnp.int32)
    for s in range(per_span):
        shift = lax.rem(offset_s[s], sectors)
        want = jnp.where(column == s, lax.rem(sector - shift + sectors, sectors), want)
        want = jnp.where(column == per_span + s, lax.rem(sector + shift, sectors), want)
        code = jnp.where(column == s, turn_s[0, s], code)
    near = jnp.zeros((PAD, LANES), F32)
    k = 0
    for piece in iface:
        for b in range(piece.shape[0] // PAD):
            near = jnp.where(want == (sector ^ k), piece[b * PAD : (b + 1) * PAD, :], near)
            k += 1
    near = turned(near, code, turn_t, stack_hi, stack_lo)
    used = small < 2 * per_span
    extra = jnp.concatenate(
        [
            jnp.where(used, near if f == 0 else pltpu.roll(near, LANES - f * 2 * per_span, 1), 0.0)
            for f in range(VALS)
        ],
        0,
    )
    one_side(2, -1, index[2:3], extra, None)
    one_side(2, 1, index[3:4], extra, None)

    ghost[0 : VALS * FACE + 1, :] = theta_ghost(th_a, slot_v)

    def theta_side(side):
        for t in range(tiles):
            cols = slice(t * LANES, (t + 1) * LANES)
            end = ORDER if side > 0 else 0
            own = [face_rows(staged, value_index(f, 0), t, 0, end) for f in range(VALS)]
            other = [ghost[f * FACE : (f + 1) * FACE, cols] for f in range(VALS)]
            for f, x in enumerate(surface(own, other, 0, side)):
                add_face_rows(acc, f, t, 0, end, x)

    odd = lax.rem(sector, 2)

    @pl.when(odd == 0)
    def _():
        theta_side(1)

    @pl.when(odd == 1)
    def _():
        theta_side(-1)

    for t in range(tiles):
        cols = slice(t * LANES, (t + 1) * LANES)
        for f in range(5):
            total = acc[f, t, 0:VOL, :]
            store_out[f, :, cols] = total
            fields_out[f, :, cols] = fields[f, :, cols] + section_gain * total


def last_kernel(odd_s, slot_v, fields, velocity, sound, store_in, fields_alias, th_b, fields_out, store_out, ghost):
    del fields_alias
    elems = slot_v.shape[1]
    tiles = elems // LANES
    ghost[...] = theta_ghost(th_b, slot_v)
    store_out[...] = store_in[...]

    def theta_side(side):
        start = (ORDER * FACE) % PAD if side > 0 else 0
        rows = slice(start, start + FACE)
        for t in range(tiles):
            cols = slice(t * LANES, (t + 1) * LANES)
            own = [fields[f, rows, cols] for f in range(5)] + [velocity[0, rows, cols], sound[rows, cols]]
            other = [ghost[f * FACE : (f + 1) * FACE, cols] for f in range(VALS)]
            for f, x in enumerate(surface(own, other, 0, side)):
                store_out[f, rows, cols] += x

    @pl.when(odd_s[0] == 0)
    def _():
        theta_side(-1)

    @pl.when(odd_s[0] == 1)
    def _():
        theta_side(1)

    for f in range(5):
        fields_out[f] = fields[f] + section_gain * store_out[f]


def params(**extra):
    return pltpu.CompilerParams(vmem_limit_bytes=VMEM_LIMIT, **extra)


def vmem_spec():
    return pl.BlockSpec(memory_space=pltpu.VMEM)


def smem_spec():
    return pl.BlockSpec(memory_space=pltpu.SMEM)


def on_device(fields, section_store, mean_velocity, sound_speed, element_slot, face_turn, rotor_offset):
    per_theta, per_span = face_turn.shape
    elems = element_slot.shape[0]
    axial = elems // (per_theta * per_span)
    sectors, slabs = lax.axis_size("blk"), lax.axis_size("span")
    tiles = elems // LANES
    assert per_theta == 1 and axial == LANES and sectors % 2 == 0 and sectors & (sectors - 1) == 0
    assert 2 * per_span * VALS < LANES
    slot_row = element_slot.reshape(1, elems)
    sds = jax.ShapeDtypeStruct
    theta_shape = sds((VALS * FACE + 1, elems), F32)
    span_shape = sds((VALS * PAD, LANES), F32)
    th_a, th_b, sp_a, sp_b, iface = pl.pallas_call(
        functools.partial(pack_kernel, per_span, axial),
        out_shape=(theta_shape, theta_shape, span_shape, span_shape, sds((PAD, LANES), F32)),
        in_specs=[smem_spec(), smem_spec()] + [vmem_spec()] * 5,
        out_specs=(vmem_spec(),) * 5,
        scratch_shapes=[
            pltpu.VMEM((9, tiles, LANES, LANES), F32),
            pltpu.VMEM((VALS * PAD, elems), BF),
            pltpu.VMEM((VALS * PAD, elems), BF),
            pltpu.VMEM((8 * PAD, LANES), BF),
            pltpu.VMEM((8 * PAD, LANES), BF),
        ],
        compiler_params=params(),
        name="pack",
    )(element_slot, face_turn, slot_row, fields, mean_velocity, sound_speed, jnp.asarray(turn_matrix(True)))

    pieces = [iface]
    near = lax.ppermute(iface, "blk", [(i, i ^ 1) for i in range(sectors)])
    near_a = lax.ppermute(th_a, "blk", [(i, i ^ 1) for i in range(sectors)])
    pairs = [(i, i + 1 if i % 2 else i - 1) for i in range(sectors)]
    near_b = lax.ppermute(th_b, "blk", [(i, j % sectors) for i, j in pairs])
    span_a = lax.ppermute(sp_a, "span", [(i, i ^ 1) for i in range(slabs) if i ^ 1 < slabs])
    pairs = [(i, i + 1 if i % 2 else i - 1) for i in range(slabs)]
    span_b = lax.ppermute(sp_b, "span", [(i, j) for i, j in pairs if 0 <= j < slabs])
    pieces.append(near)
    reach = 2
    while reach < sectors:
        block = jnp.concatenate(pieces, 0)
        pieces.append(lax.ppermute(block, "blk", [(i, i ^ reach) for i in range(sectors)]))
        reach *= 2

    width = 2 * LANES
    state = lambda: pl.BlockSpec((5, VOL, width), lambda i: (0, 0, i))
    part = pl.pallas_call(
        volume_kernel,
        grid=(elems // width,),
        out_shape=sds((5, VOL, elems), F32),
        in_specs=[
            state(),
            pl.BlockSpec((3, VOL, width), lambda i: (0, 0, i)),
            pl.BlockSpec((VOL, width), lambda i: (0, i)),
            state(),
            pl.BlockSpec((2 * LANES, 3 * LANES), lambda i: (0, 0)),
        ],
        out_specs=state(),
        scratch_shapes=[pltpu.VMEM((5, 3 * LANES, width), BF), pltpu.VMEM((5, 3 * LANES, width), BF)],
        compiler_params=params(),
        cost_estimate=pl.CostEstimate(flops=2 * 5 * 384 * 384 * elems, bytes_accessed=6 * 10**6, transcendentals=0),
        name="volume",
    )(fields, mean_velocity, sound_speed, section_store, jnp.asarray(volume_matrix()))

    whole = sds((5, VOL, elems), F32)
    fields_part, store_part = pl.pallas_call(
        functools.partial(face_kernel, per_span, axial, sectors, slabs, len(pieces)),
        out_shape=(whole, whole),
        in_specs=[smem_spec(), smem_spec()] + [vmem_spec()] * (9 + len(pieces)),
        out_specs=(vmem_spec(),) * 2,
        scratch_shapes=[
            pltpu.VMEM((9, tiles, LANES, LANES), F32),
            pltpu.VMEM((5, tiles, LANES, LANES), F32),
            pltpu.VMEM((VALS * PAD, elems + LANES), BF),
            pltpu.VMEM((VALS * PAD, elems + LANES), BF),
            pltpu.VMEM((8 * PAD, LANES), BF),
            pltpu.VMEM((8 * PAD, LANES), BF),
            pltpu.VMEM((VALS * PAD, elems), F32),
        ],
        compiler_params=params(),
        name="faces",
    )(
        rotor_offset, face_turn, slot_row, fields, mean_velocity, sound_speed, part, near_a, span_a, span_b,
        jnp.asarray(turn_matrix(False)), *pieces,
    )

    odd = lax.rem(lax.axis_index("blk"), 2).astype(jnp.int32).reshape(1)
    last = (VOL - 1) // PAD

    def window(lead):
        return pl.BlockSpec(lead + (PAD, elems), lambda i, o: (0,) * len(lead) + (o[0] * last, 0))

    return pl.pallas_call(
        last_kernel,
        out_shape=(whole, whole),
        grid_spec=pltpu.PrefetchScalarGridSpec(
            num_scalar_prefetch=1,
            grid=(1,),
            in_specs=[
                pl.BlockSpec((1, elems), lambda i, o: (0, 0)),
                window((5,)),
                window((1,)),
                window(()),
                window((5,)),
                pl.BlockSpec(memory_space=pl.ANY),
                pl.BlockSpec((VALS * FACE + 1, elems), lambda i, o: (0, 0)),
            ],
            out_specs=(window((5,)), window((5,))),
            scratch_shapes=[pltpu.VMEM((VALS * FACE + 1, elems), F32)],
        ),
        input_output_aliases={5: 1, 6: 0},
        compiler_params=params(),
        name="last",
    )(odd, slot_row, fields, mean_velocity, sound_speed, store_part, fields_part, near_b)


def solution(mesh):
    both = ("blk", "span")
    in_specs = (
        P(None, None, both),
        P(None, None, both),
        P(None, None, both),
        P(None, both),
        P(both),
        P("blk", "span"),
        P("span"),
    )
    out_specs = (P(None, None, both), P(None, None, both))
    return jax.shard_map(on_device, mesh=mesh, in_specs=in_specs, out_specs=out_specs, check_vma=False)
```

```python
import functools

import jax
import jax.numpy as jnp
import numpy as np
from jax import lax
from jax.experimental import pallas as pl
from jax.experimental.pallas import tpu as pltpu
from jax.sharding import PartitionSpec as P


ORDER = 4
NODE = ORDER + 1
FACE = NODE * NODE
VOL = NODE**3
LANES = 128
PAD = 32
VALS = 7

section_decay = -567301805773.0 / 1357537059087.0
section_gain = 5161836677717.0 / 13612068292357.0
time_step = 0.05
metric_scale = (1.0, 1.5, 0.75)
end_weight = 0.1

BF = jnp.bfloat16
F32 = jnp.float32
VMEM_LIMIT = 24 * 1024 * 1024


def lobatto_slopes():
    inner_root = np.sqrt(3.0 / 7.0)
    points = np.array([-1.0, -inner_root, 0.0, inner_root, 1.0])
    count = points.shape[0]
    slopes = np.zeros((count, count))
    for r in range(count):
        for c in range(count):
            if r == c:
                slopes[r, c] = sum(1.0 / (points[r] - points[o]) for o in range(count) if o != r)
            else:
                top = np.prod([points[r] - points[o] for o in range(count) if o != r])
                low = np.prod([points[c] - points[o] for o in range(count) if o != c])
                slopes[r, c] = top / (low * (points[r] - points[c]))
    return slopes


def split_np(table):
    high = np.asarray(table, np.float32).astype(BF)
    low = (np.asarray(table, np.float64) - high.astype(np.float64)).astype(BF)
    return high, low


def volume_matrix():
    slopes = lobatto_slopes()
    eye = np.eye(NODE)
    parts = (
        np.kron(np.kron(slopes, eye), eye),
        np.kron(np.kron(eye, slopes), eye),
        np.kron(np.kron(eye, eye), slopes),
    )
    full = np.zeros((LANES, 3 * LANES))
    for d in range(3):
        full[:VOL, d * LANES : d * LANES + VOL] = -time_step * metric_scale[d] * parts[d]
    high, low = split_np(full)
    return np.concatenate([high, low], 0)


def turn_matrix(inverse):
    table = np.zeros((PAD, 8 * PAD), np.float32)
    for code in range(8):
        index = np.arange(FACE).reshape(NODE, NODE)
        if inverse:
            if code & 2:
                index = index[:, ::-1]
            if code & 1:
                index = index[::-1, :]
            if code & 4:
                index = index.T
        else:
            if code & 4:
                index = index.T
            if code & 1:
                index = index[::-1, :]
            if code & 2:
                index = index[:, ::-1]
        for n, o in enumerate(index.reshape(-1)):
            table[n, code * PAD + o] = 1.0
    return table.astype(BF)


def dot(a, b):
    return jnp.dot(a, b, preferred_element_type=F32)


def dot_t(a, b):
    return lax.dot_general(a, b, (((1,), (1,)), ((), ())), preferred_element_type=F32)


def halves(x):
    high = x.astype(BF)
    return high, (x - high.astype(F32)).astype(BF)


def lane_iota(shape):
    return lax.broadcasted_iota(jnp.int32, shape, len(shape) - 1)


def row_iota(shape):
    return lax.broadcasted_iota(jnp.int32, shape, 0)


def face_rows(ref, v, tile, d, end):
    if d == 0:
        return ref[v, tile, pl.ds(end * FACE, FACE), :]
    if d == 1:
        starts = [i * FACE + end * NODE for i in range(NODE)]
        return jnp.concatenate([ref[v, tile, pl.ds(s, NODE), :] for s in starts], axis=0)
    return ref[v, tile, pl.ds(end, FACE, NODE), :]


def add_face_rows(ref, v, tile, d, end, value):
    if d == 0:
        ref[v, tile, pl.ds(end * FACE, FACE), :] += value
    elif d == 1:
        for i in range(NODE):
            ref[v, tile, pl.ds(i * FACE + end * NODE, NODE), :] += value[i * NODE : (i + 1) * NODE]
    else:
        ref[v, tile, pl.ds(end, FACE, NODE), :] += value


def value_index(f, d):
    return f if f < 5 else (5 + d if f == 5 else 8)


def surface(own, other, d, side):
    qo, mo, co = own[:5], own[5], own[6]
    qn, mn, cn = other[:5], other[5], other[6]
    reach = jnp.maximum(jnp.abs(mo) + co, jnp.abs(mn) + cn)
    weight = side * 0.5 * time_step * metric_scale[d] / end_weight
    if side > 0:
        ao, an = mo - reach, mn - reach
    else:
        ao, an = mo + reach, mn + reach
    velocity_part = co * qo[1 + d] - cn * qn[1 + d]
    pressure_part = co * qo[4] - cn * qn[4]
    out = []
    for f in range(5):
        x = ao * qo[f] - an * qn[f]
        if f in (0, 4):
            x = x + velocity_part
        elif f == 1 + d:
            x = x + pressure_part
        out.append(weight * x)
    return out


def axis_parity(axis):
    return lax.rem(lax.axis_index(axis), 2)


def one_hot(index_row, count):
    return (row_iota((count, index_row.shape[1])) == index_row).astype(BF)


def store_halves(ref_hi, ref_lo, at, cols, value):
    hi, lo = halves(jnp.concatenate([value, jnp.zeros((PAD - FACE, value.shape[1]), F32)], 0))
    ref_hi[at : at + PAD, cols] = hi
    ref_lo[at : at + PAD, cols] = lo


def turned(packed, code, turn_t, stack_hi, stack_lo):
    hi = packed.astype(BF).astype(F32)
    lo = packed - hi
    for c in range(8):
        stack_hi[c * PAD : (c + 1) * PAD, :] = jnp.where(code == c, hi, 0.0).astype(BF)
        stack_lo[c * PAD : (c + 1) * PAD, :] = jnp.where(code == c, lo, 0.0).astype(BF)
    return dot(turn_t[...], stack_hi[...]) + dot(turn_t[...], stack_lo[...])


def tile_cols(t):
    return slice(t * LANES, (t + 1) * LANES)


def neighbour_index(rows, slot_v):
    elems = slot_v.shape[1]
    own = (row_iota((elems, elems)) == slot_v[...]).astype(BF)
    base = 256.0
    table = jnp.concatenate(rows + [jnp.zeros((8 - len(rows), elems), F32)], 0)
    upper = jnp.floor(table * (1.0 / base))
    lower = table - upper * base
    both = jnp.concatenate([upper, lower], 0).astype(BF)
    moved = dot_t(both, own)
    return (moved[0:8] * base + moved[8:16]).astype(jnp.int32)


def first_kernel(
    per_span, axial, slot_s, turn_s, slot_h, fields, velocity, sound, turn_h,
    staged, th_a, iface, slot_v, theta, turn_t, rows_hi, rows_lo, stack_hi, stack_lo, sems, small_sems, out_sem,
):
    elems = slot_v.shape[1]
    tiles = elems // LANES
    half = axial // 2
    rows = VALS * PAD
    small = [
        pltpu.make_async_copy(slot_h, slot_v, small_sems.at[0]),
        pltpu.make_async_copy(turn_h, turn_t, small_sems.at[1]),
    ]
    loads = []
    for t in range(tiles):
        cols = pl.ds(t * LANES, LANES)
        loads.append([
            pltpu.make_async_copy(fields.at[:, :, cols], staged.at[0:5, t, 0:VOL, :], sems.at[t, 0]),
            pltpu.make_async_copy(velocity.at[:, :, cols], staged.at[5:8, t, 0:VOL, :], sems.at[t, 1]),
            pltpu.make_async_copy(sound.at[:, cols], staged.at[8, t, 0:VOL, :], sems.at[t, 2]),
        ])
        for copy in loads[-1]:
            copy.start()
    for copy in small:
        copy.start()
    lane = lane_iota((1, LANES))
    column = lane % (2 * per_span)
    target = jnp.full((1, LANES), -1, jnp.int32)
    code = jnp.zeros((1, LANES), jnp.int32)
    for s in range(per_span):
        target = jnp.where(lane == s, slot_s[s * axial + half - 1], target)
        target = jnp.where(lane == per_span + s, slot_s[s * axial + half], target)
        code = jnp.where(column == per_span + s, turn_s[0, s], code)
    one = one_hot(target, elems)
    theta[VALS * FACE : VALS * FACE + 1, :] = jnp.zeros((1, elems), F32)
    odd = axis_parity("blk")

    for t in range(tiles):
        for copy in loads[t]:
            copy.wait()
        cols = tile_cols(t)

        @pl.when(odd == 0)
        def _():
            for f in range(VALS):
                theta[f * FACE : (f + 1) * FACE, cols] = face_rows(staged, value_index(f, 0), t, 0, ORDER)

        @pl.when(odd == 1)
        def _():
            for f in range(VALS):
                theta[f * FACE : (f + 1) * FACE, cols] = face_rows(staged, value_index(f, 0), t, 0, 0)

        for n, end in enumerate((ORDER, 0)):
            for f in range(VALS):
                at = n * rows + f * PAD
                store_halves(rows_hi, rows_lo, at, cols, face_rows(staged, value_index(f, 2), t, 2, end))
    out = pltpu.make_async_copy(theta, th_a, out_sem)
    out.start()
    for copy in small:
        copy.wait()
    both = dot(rows_hi[...], one) + dot(rows_lo[...], one)
    both = jnp.where(lane < per_span, both[0:rows], jnp.where(lane < 2 * per_span, both[rows:], 0.0))
    packed = both[0:PAD]
    for f in range(1, VALS):
        packed = packed + pltpu.roll(both[f * PAD : (f + 1) * PAD], f * 2 * per_span, 1)
    iface[...] = turned(packed, code, turn_t, stack_hi, stack_lo)
    for t in range(tiles):
        iface[PAD - tiles + t : PAD - tiles + t + 1, :] = slot_v[:, tile_cols(t)].astype(F32)
    out.wait()


LOCAL_FACES = ((1, 1), (1, 0), (2, 1), (2, 0))


def second_kernel(
    per_span, axial, slot_v, staged, th_b, sp_a, sp_b, index, rows_hi, rows_lo, theta, out_sem,
):
    elems = slot_v.shape[1]
    tiles = elems // LANES
    half = axial // 2
    rows = VALS * PAD
    theta[VALS * FACE : VALS * FACE + 1, :] = jnp.zeros((1, elems), F32)
    odd = axis_parity("blk")

    @pl.when(odd == 0)
    def _():
        for t in range(tiles):
            for f in range(VALS):
                theta[f * FACE : (f + 1) * FACE, tile_cols(t)] = face_rows(staged, value_index(f, 0), t, 0, 0)

    @pl.when(odd == 1)
    def _():
        for t in range(tiles):
            for f in range(VALS):
                theta[f * FACE : (f + 1) * FACE, tile_cols(t)] = face_rows(staged, value_index(f, 0), t, 0, ORDER)

    out = pltpu.make_async_copy(theta, th_b, out_sem)
    out.start()
    for n, (d, end) in enumerate(LOCAL_FACES):
        for t in range(tiles):
            for f in range(VALS):
                x = face_rows(staged, value_index(f, d), t, d, end * ORDER)
                store_halves(rows_hi, rows_lo, n * rows + f * PAD, tile_cols(t), x)

    def gathered(start, row):
        one = one_hot(row, elems)
        return dot(rows_hi[start : start + rows, :], one) + dot(rows_lo[start : start + rows, :], one)

    high = gathered(0, slot_v[:, elems - axial : elems])
    low = gathered(rows, slot_v[:, 0:axial])
    span_odd = axis_parity("span")

    @pl.when(span_odd == 0)
    def _():
        sp_a[...] = high
        sp_b[...] = low

    @pl.when(span_odd == 1)
    def _():
        sp_a[...] = low
        sp_b[...] = high

    slots = slot_v[...].astype(F32)
    lane = lane_iota((1, elems))
    position = lane % axial
    row = (lane // axial).astype(F32)
    lanes_f = lane.astype(F32)
    span_low = jnp.where(lane < axial, elems + lanes_f, pltpu.roll(slots, axial, 1))
    span_high = jnp.where(lane >= elems - axial, axial + lanes_f, pltpu.roll(slots, elems - axial, 1))
    none = elems + LANES - 1.0
    ax_low = jnp.where(position == half, elems + row, pltpu.roll(slots, 1, 1))
    ax_low = jnp.where(position == 0, none, ax_low)
    ax_high = jnp.where(position == half - 1, elems + per_span + row, pltpu.roll(slots, elems - 1, 1))
    ax_high = jnp.where(position == axial - 1, none, ax_high)
    index[...] = neighbour_index([span_low, span_high, ax_low, ax_high], slot_v)
    out.wait()


def local_kernel(index, rows_hi, rows_lo, ghosts):
    elems = index.shape[1]
    rows = VALS * PAD
    for n in range(len(LOCAL_FACES)):
        one = one_hot(index[n : n + 1, :], elems)
        at = slice(n * rows, (n + 1) * rows)
        ghosts[n] = dot(rows_hi[at, :], one) + dot(rows_lo[at, :], one)


def volume_kernel(staged, store_h, matrix_h, out, store, matrix, flux_hi, flux_lo, sems):
    tiles = staged.shape[1]
    loads = [pltpu.make_async_copy(matrix_h, matrix, sems.at[tiles])]
    for t in range(tiles):
        loads.append(pltpu.make_async_copy(store_h.at[:, :, pl.ds(t * LANES, LANES)], store.at[:, t, 0:VOL, :], sems.at[t]))
    for copy in loads:
        copy.start()
    step = 16
    for pair in range(tiles // 2):
        for half in range(2):
            t = 2 * pair + half
            cols = tile_cols(half)
            for r in range(0, VOL, step):
                n = min(step, VOL - r)
                rows = slice(r, r + n)
                q = [staged[f, t, rows, :] for f in range(5)]
                c = staged[8, t, rows, :]
                cp = c * q[4]
                for d in range(3):
                    m = staged[5 + d, t, rows, :]
                    cu = c * q[1 + d]
                    for f in range(5):
                        x = m * q[f]
                        if f in (0, 4):
                            x = x + cu
                        elif f == 1 + d:
                            x = x + cp
                        if n < step:
                            x = jnp.concatenate([x, jnp.zeros((step - n, LANES), F32)], 0)
                        hi, lo = halves(x)
                        flux_hi[f, d * LANES + r : d * LANES + r + step, cols] = hi
                        flux_lo[f, d * LANES + r : d * LANES + r + step, cols] = lo
        if pair == 0:
            for copy in loads:
                copy.wait()
        for f in range(5):
            a = dot(matrix[...], flux_hi[f])
            b = dot(matrix[0:LANES, :], flux_lo[f])
            total = a[0:LANES] + a[LANES : 2 * LANES] + b
            for half in range(2):
                t = 2 * pair + half
                out[f, t, 0:VOL, :] = section_decay * store[f, t, 0:VOL, :] + total[0:VOL, tile_cols(half)]


def theta_ghost(recv, index_row):
    one = one_hot(index_row, recv.shape[1])
    hi, lo = halves(recv[...])
    return dot(hi, one) + dot(lo, one)


def theta_side(staged, ghost, acc, shift, side):
    start = ORDER * FACE if side > 0 else 0
    for t in range(staged.shape[1]):
        own = [staged[value_index(f, 0), t, start : start + FACE, :] for f in range(VALS)]
        other = [ghost[f * FACE : (f + 1) * FACE, tile_cols(t)] for f in range(VALS)]
        for f, x in enumerate(surface(own, other, 0, side)):
            acc[f, t, start - shift : start - shift + FACE, :] += x


HIGH_ROW = (ORDER * FACE) // PAD * PAD


def face_kernel(
    per_span, sectors, slabs, pieces,
    offset_s, turn_s, slot_v, staged, part, index, ghosts, th_a, sp_a, sp_b, turn_h, *rest,
):
    iface = rest[:pieces]
    fields_out, store_out, window, index_b = rest[pieces : pieces + 4]
    acc, fresh, turn_t, stack_hi, stack_lo, ghost, sems, small_sem = rest[pieces + 4 :]
    elems = slot_v.shape[1]
    tiles = elems // LANES
    load = pltpu.make_async_copy(turn_h, turn_t, small_sem)
    load.start()
    sector = lax.axis_index("blk")
    odd = lax.rem(sector, 2)

    partner = lax.rem(sector + jnp.where(odd == 1, 1, sectors - 1), sectors)
    slots_a = iface[1][PAD - tiles : PAD, :]
    slots_b = jnp.zeros((tiles, LANES), F32)
    small = lane_iota((1, LANES))
    column = small % (2 * per_span)
    want = jnp.zeros((1, LANES), jnp.int32)
    code = jnp.zeros((1, LANES), jnp.int32)
    for s in range(per_span):
        shift = lax.rem(offset_s[s], sectors)
        want = jnp.where(column == s, lax.rem(sector - shift + sectors, sectors), want)
        want = jnp.where(column == per_span + s, lax.rem(sector + shift, sectors), want)
        code = jnp.where(column == s, turn_s[0, s], code)
    near = jnp.zeros((PAD, LANES), F32)
    k = 0
    for piece in iface:
        for b in range(piece.shape[0] // PAD):
            block = piece[b * PAD : (b + 1) * PAD, :]
            near = jnp.where(want == (sector ^ k), block, near)
            slots_b = jnp.where(partner == (sector ^ k), block[PAD - tiles :], slots_b)
            k += 1
    flat = lambda x: jnp.concatenate([x[t : t + 1] for t in range(tiles)], 1)
    theta_index = neighbour_index([flat(slots_a), flat(slots_b)], slot_v)
    index_b[...] = theta_index

    for t in range(tiles):
        for f in range(5):
            acc[f, t, 0:VOL, :] = part[f, t, 0:VOL, :]
    ghost[...] = theta_ghost(th_a, theta_index[0:1])

    @pl.when(odd == 0)
    def _():
        theta_side(staged, ghost, acc, 0, 1)

    @pl.when(odd == 1)
    def _():
        theta_side(staged, ghost, acc, 0, -1)

    def one_side(n, d, side, extra, wall, after=None):
        end = ORDER if side > 0 else 0
        index_row = index[n : n + 1, :]
        hi, lo = halves(extra)
        one = one_hot(index_row - elems, LANES)
        other_all = ghosts[n] + (dot(hi, one) + dot(lo, one))
        for t in range(tiles):
            cols = tile_cols(t)
            own = [face_rows(staged, value_index(f, d), t, d, end) for f in range(VALS)]
            other = [other_all[f * PAD : f * PAD + FACE, cols] for f in range(VALS)]
            if wall is not None:
                at_wall = jnp.logical_and(index_row[:, cols] >= elems, wall)
                for f in range(VALS):
                    other[f] = jnp.where(at_wall, -own[f] if f == 1 + d else own[f], other[f])
            for f, x in enumerate(surface(own, other, d, side)):
                add_face_rows(acc, f, t, d, end, x)
            if after is not None:
                after(t)

    slab = lax.axis_index("span")
    slab_odd = lax.rem(slab, 2) == 1
    one_side(0, 1, -1, jnp.where(slab_odd, sp_a[...], sp_b[...]), slab == 0)
    one_side(1, 1, 1, jnp.where(slab_odd, sp_b[...], sp_a[...]), slab == slabs - 1)

    load.wait()
    near = turned(near, code, turn_t, stack_hi, stack_lo)
    used = small < 2 * per_span
    extra = jnp.concatenate(
        [
            jnp.where(used, near if f == 0 else pltpu.roll(near, LANES - f * 2 * per_span, 1), 0.0)
            for f in range(VALS)
        ],
        0,
    )
    one_side(2, 2, -1, extra, None)

    def copies(t, low, high):
        cols = pl.ds(t * LANES, LANES)
        return (
            pltpu.make_async_copy(acc.at[:, t, low:high, :], store_out.at[:, low:high, cols], sems.at[t, 0]),
            pltpu.make_async_copy(fresh.at[:, t, low:high, :], fields_out.at[:, low:high, cols], sems.at[t, 1]),
        )

    def finish(t):
        for f in range(5):
            fresh[f, t, 0:VOL, :] = staged[f, t, 0:VOL, :] + section_gain * acc[f, t, 0:VOL, :]

        @pl.when(odd == 0)
        def _():
            for f in range(5):
                window[f, t] = acc[f, t, 0:PAD, :]
            for copy in copies(t, PAD, VOL):
                copy.start()

        @pl.when(odd == 1)
        def _():
            for f in range(5):
                window[f, t, 0 : VOL - HIGH_ROW] = acc[f, t, HIGH_ROW:VOL, :]
            for copy in copies(t, 0, HIGH_ROW):
                copy.start()

    one_side(3, 2, 1, extra, None, finish)

    @pl.when(odd == 0)
    def _():
        for t in range(tiles):
            for copy in copies(t, PAD, VOL):
                copy.wait()

    @pl.when(odd == 1)
    def _():
        for t in range(tiles):
            for copy in copies(t, 0, HIGH_ROW):
                copy.wait()


def last_kernel(index_b, staged, window, th_b, fields_in, store_in, fields_out, store_out, ghost, acc, fresh, sems):
    del fields_in, store_in
    tiles = staged.shape[1]
    ghost[...] = theta_ghost(th_b, index_b[1:2])
    acc[...] = window[...]

    def finish(side, low, high):
        theta_side(staged, ghost, acc, low, side)
        copies = []
        for t in range(tiles):
            for f in range(5):
                fresh[f, t, 0 : high - low, :] = (
                    staged[f, t, low:high, :] + section_gain * acc[f, t, 0 : high - low, :]
                )
            cols = pl.ds(t * LANES, LANES)
            pair = (
                pltpu.make_async_copy(acc.at[:, t, 0 : high - low, :], store_out.at[:, low:high, cols], sems.at[t, 0]),
                pltpu.make_async_copy(fresh.at[:, t, 0 : high - low, :], fields_out.at[:, low:high, cols], sems.at[t, 1]),
            )
            for copy in pair:
                copy.start()
            copies.extend(pair)
        for copy in copies:
            copy.wait()

    odd = axis_parity("blk")

    @pl.when(odd == 0)
    def _():
        finish(-1, 0, PAD)

    @pl.when(odd == 1)
    def _():
        finish(1, HIGH_ROW, VOL)


def params(limit=VMEM_LIMIT):
    return pltpu.CompilerParams(vmem_limit_bytes=limit)


def vmem_spec():
    return pl.BlockSpec(memory_space=pltpu.VMEM)


def hbm_spec():
    return pl.BlockSpec(memory_space=pltpu.HBM)


def smem_spec():
    return pl.BlockSpec(memory_space=pltpu.SMEM)


def in_hbm(x):
    return pltpu.with_memory_space_constraint(x, pltpu.HBM)


def in_vmem(x):
    return pltpu.with_memory_space_constraint(x, pltpu.VMEM)


def on_device(fields, section_store, mean_velocity, sound_speed, element_slot, face_turn, rotor_offset):
    per_theta, per_span = face_turn.shape
    elems = element_slot.shape[0]
    axial = elems // (per_theta * per_span)
    sectors, slabs = lax.axis_size("blk"), lax.axis_size("span")
    tiles = elems // LANES
    rows = VALS * PAD
    assert per_theta == 1 and axial == LANES and sectors % 2 == 0 and sectors & (sectors - 1) == 0
    assert 2 * per_span * VALS < LANES and FACE + tiles <= PAD
    dma = pltpu.SemaphoreType.DMA
    theta_rows = VALS * FACE + 1
    vmem, hbm = pltpu.VMEM, pltpu.HBM
    slot_h = in_hbm(element_slot.reshape(1, elems))
    stack = [vmem((8 * PAD, LANES), BF), vmem((8 * PAD, LANES), BF)]
    staged, th_a, iface, slot_v = pl.pallas_call(
        functools.partial(first_kernel, per_span, axial),
        out_shape=(
            vmem((9, tiles, LANES, LANES), F32),
            hbm((theta_rows, elems), F32),
            vmem((PAD, LANES), F32),
            vmem((1, elems), jnp.int32),
        ),
        in_specs=[smem_spec(), smem_spec()] + [hbm_spec()] * 5,
        out_specs=(vmem_spec(), hbm_spec(), vmem_spec(), vmem_spec()),
        scratch_shapes=[
            vmem((theta_rows, elems), F32),
            vmem((PAD, 8 * PAD), BF),
            vmem((2 * rows, elems), BF),
            vmem((2 * rows, elems), BF),
            *stack,
            dma((tiles, 3)),
            dma((2,)),
            dma(()),
        ],
        compiler_params=params(),
        name="first",
    )(
        in_hbm(element_slot), in_hbm(face_turn), slot_h, in_hbm(fields), in_hbm(mean_velocity), in_hbm(sound_speed),
        in_hbm(jnp.asarray(turn_matrix(True))),
    )

    pieces = [iface]
    pieces.append(lax.ppermute(iface, "blk", [(i, i ^ 1) for i in range(sectors)]))
    near_a = lax.ppermute(th_a, "blk", [(i, i ^ 1) for i in range(sectors)])
    reach = 2
    while reach < sectors:
        block = jnp.concatenate(pieces, 0)
        pieces.append(lax.ppermute(block, "blk", [(i, i ^ reach) for i in range(sectors)]))
        reach *= 2

    th_b, sp_a, sp_b, index, rows_hi, rows_lo = pl.pallas_call(
        functools.partial(second_kernel, per_span, axial),
        out_shape=(
            hbm((theta_rows, elems), F32),
            vmem((rows, LANES), F32),
            vmem((rows, LANES), F32),
            vmem((8, elems), jnp.int32),
            vmem((len(LOCAL_FACES) * rows, elems), BF),
            vmem((len(LOCAL_FACES) * rows, elems), BF),
        ),
        in_specs=[vmem_spec()] * 2,
        out_specs=(hbm_spec(),) + (vmem_spec(),) * 5,
        scratch_shapes=[vmem((theta_rows, elems), F32), dma(())],
        compiler_params=params(),
        name="second",
    )(in_vmem(slot_v), in_vmem(staged))
    pairs = [(i, (i + 1 if i % 2 else i - 1) % sectors) for i in range(sectors)]
    near_b = lax.ppermute(th_b, "blk", pairs)
    span_a = lax.ppermute(sp_a, "span", [(i, i ^ 1) for i in range(slabs) if i ^ 1 < slabs])
    pairs = [(i, i + 1 if i % 2 else i - 1) for i in range(slabs)]
    span_b = lax.ppermute(sp_b, "span", [(i, j) for i, j in pairs if 0 <= j < slabs])

    ghosts = pl.pallas_call(
        local_kernel,
        out_shape=vmem((len(LOCAL_FACES), rows, elems), F32),
        in_specs=[vmem_spec()] * 3,
        out_specs=vmem_spec(),
        compiler_params=params(),
        name="local",
    )(in_vmem(index), in_vmem(rows_hi), in_vmem(rows_lo))

    part = pl.pallas_call(
        volume_kernel,
        out_shape=vmem((5, tiles, LANES, LANES), F32),
        in_specs=[vmem_spec()] + [hbm_spec()] * 2,
        out_specs=vmem_spec(),
        scratch_shapes=[
            vmem((5, tiles, LANES, LANES), F32),
            vmem((2 * LANES, 3 * LANES), BF),
            vmem((5, 3 * LANES, 2 * LANES), BF),
            vmem((5, 3 * LANES, 2 * LANES), BF),
            dma((tiles + 1,)),
        ],
        compiler_params=params(),
        name="volume",
    )(in_vmem(staged), in_hbm(section_store), in_hbm(jnp.asarray(volume_matrix())))

    whole = hbm((5, VOL, elems), F32)
    fields_part, store_part, window, index_b = pl.pallas_call(
        functools.partial(face_kernel, per_span, sectors, slabs, len(pieces)),
        out_shape=(whole, whole, vmem((5, tiles, PAD, LANES), F32), vmem((8, elems), jnp.int32)),
        in_specs=[smem_spec(), smem_spec()] + [vmem_spec()] * 8 + [hbm_spec()] + [vmem_spec()] * len(pieces),
        out_specs=(hbm_spec(),) * 2 + (vmem_spec(),) * 2,
        scratch_shapes=[
            vmem((5, tiles, LANES, LANES), F32),
            vmem((5, tiles, LANES, LANES), F32),
            vmem((PAD, 8 * PAD), BF),
            *stack,
            vmem((theta_rows, elems), F32),
            dma((tiles, 2)),
            dma(()),
        ],
        compiler_params=params(),
        name="faces",
    )(
        in_hbm(rotor_offset), in_hbm(face_turn), in_vmem(slot_v), in_vmem(staged), in_vmem(part), in_vmem(index),
        in_vmem(ghosts), in_vmem(near_a), in_vmem(span_a), in_vmem(span_b), in_hbm(jnp.asarray(turn_matrix(False))),
        *[in_vmem(piece) for piece in pieces],
    )

    return pl.pallas_call(
        last_kernel,
        out_shape=(whole, whole),
        in_specs=[vmem_spec()] * 4 + [hbm_spec()] * 2,
        out_specs=(hbm_spec(),) * 2,
        scratch_shapes=[
            vmem((theta_rows, elems), F32),
            vmem((5, tiles, PAD, LANES), F32),
            vmem((5, tiles, PAD, LANES), F32),
            dma((tiles, 2)),
        ],
        input_output_aliases={4: 0, 5: 1},
        compiler_params=params(),
        name="last",
    )(in_vmem(index_b), in_vmem(staged), in_vmem(window), in_vmem(near_b), fields_part, store_part)


def solution(mesh):
    both = ("blk", "span")
    in_specs = (
        P(None, None, both),
        P(None, None, both),
        P(None, None, both),
        P(None, both),
        P(both),
        P("blk", "span"),
        P("span"),
    )
    out_specs = (P(None, None, both), P(None, None, both))
    return jax.shard_map(on_device, mesh=mesh, in_specs=in_specs, out_specs=out_specs, check_vma=False)
```

```python
import functools

import jax
import jax.numpy as jnp
import numpy as np
from jax import lax
from jax.experimental import pallas as pl
from jax.experimental.pallas import tpu as pltpu
from jax.sharding import PartitionSpec as P


ORDER = 4
NODE = ORDER + 1
FACE = NODE * NODE
VOL = NODE**3
LANES = 128
PAD = 32
VALS = 7

section_decay = -567301805773.0 / 1357537059087.0
section_gain = 5161836677717.0 / 13612068292357.0
time_step = 0.05
metric_scale = (1.0, 1.5, 0.75)
end_weight = 0.1

BF = jnp.bfloat16
F32 = jnp.float32
VMEM_LIMIT = 24 * 1024 * 1024


def lobatto_slopes():
    inner_root = np.sqrt(3.0 / 7.0)
    points = np.array([-1.0, -inner_root, 0.0, inner_root, 1.0])
    count = points.shape[0]
    slopes = np.zeros((count, count))
    for r in range(count):
        for c in range(count):
            if r == c:
                slopes[r, c] = sum(1.0 / (points[r] - points[o]) for o in range(count) if o != r)
            else:
                top = np.prod([points[r] - points[o] for o in range(count) if o != r])
                low = np.prod([points[c] - points[o] for o in range(count) if o != c])
                slopes[r, c] = top / (low * (points[r] - points[c]))
    return slopes


def split_np(table):
    high = np.asarray(table, np.float32).astype(BF)
    low = (np.asarray(table, np.float64) - high.astype(np.float64)).astype(BF)
    return high, low


def volume_matrix():
    slopes = lobatto_slopes()
    eye = np.eye(NODE)
    parts = (
        np.kron(np.kron(slopes, eye), eye),
        np.kron(np.kron(eye, slopes), eye),
        np.kron(np.kron(eye, eye), slopes),
    )
    full = np.zeros((LANES, 3 * LANES))
    for d in range(3):
        full[:VOL, d * LANES : d * LANES + VOL] = -time_step * metric_scale[d] * parts[d]
    high, low = split_np(full)
    return np.concatenate([high, low], 0)


def turn_matrix(inverse):
    table = np.zeros((PAD, 8 * PAD), np.float32)
    for code in range(8):
        index = np.arange(FACE).reshape(NODE, NODE)
        if inverse:
            if code & 2:
                index = index[:, ::-1]
            if code & 1:
                index = index[::-1, :]
            if code & 4:
                index = index.T
        else:
            if code & 4:
                index = index.T
            if code & 1:
                index = index[::-1, :]
            if code & 2:
                index = index[:, ::-1]
        for n, o in enumerate(index.reshape(-1)):
            table[n, code * PAD + o] = 1.0
    return table.astype(BF)


def dot(a, b):
    return jnp.dot(a, b, preferred_element_type=F32)


def dot_t(a, b):
    return lax.dot_general(a, b, (((1,), (1,)), ((), ())), preferred_element_type=F32)


def halves(x):
    high = x.astype(BF)
    return high, (x - high.astype(F32)).astype(BF)


def lane_iota(shape):
    return lax.broadcasted_iota(jnp.int32, shape, len(shape) - 1)


def face_rows(ref, v, tile, d, end):
    if d == 0:
        return ref[v, tile, pl.ds(end * FACE, FACE), :]
    if d == 1:
        starts = [i * FACE + end * NODE for i in range(NODE)]
        return jnp.concatenate([ref[v, tile, pl.ds(s, NODE), :] for s in starts], axis=0)
    return ref[v, tile, pl.ds(end, FACE, NODE), :]


def add_face_rows(ref, v, tile, d, end, value):
    if d == 0:
        ref[v, tile, pl.ds(end * FACE, FACE), :] += value
    elif d == 1:
        for i in range(NODE):
            ref[v, tile, pl.ds(i * FACE + end * NODE, NODE), :] += value[i * NODE : (i + 1) * NODE]
    else:
        ref[v, tile, pl.ds(end, FACE, NODE), :] += value


def value_index(f, d):
    return f if f < 5 else (5 + d if f == 5 else 8)


def surface(own, other, d, side):
    qo, mo, co = own[:5], own[5], own[6]
    qn, mn, cn = other[:5], other[5], other[6]
    reach = jnp.maximum(jnp.abs(mo) + co, jnp.abs(mn) + cn)
    weight = side * 0.5 * time_step * metric_scale[d] / end_weight
    if side > 0:
        ao, an = mo - reach, mn - reach
    else:
        ao, an = mo + reach, mn + reach
    velocity_part = co * qo[1 + d] - cn * qn[1 + d]
    pressure_part = co * qo[4] - cn * qn[4]
    out = []
    for f in range(5):
        x = ao * qo[f] - an * qn[f]
        if f in (0, 4):
            x = x + velocity_part
        elif f == 1 + d:
            x = x + pressure_part
        out.append(weight * x)
    return out


def axis_parity(axis):
    return lax.rem(lax.axis_index(axis), 2)


def one_hot(index_row, count):
    short = jnp.broadcast_to(index_row, (16, index_row.shape[1])).astype(jnp.int16)
    rows = lax.broadcasted_iota(jnp.int16, (16, index_row.shape[1]), 0)
    one, zero = jnp.ones(short.shape, BF), jnp.zeros(short.shape, BF)
    return jnp.concatenate([jnp.where(rows == short - r, one, zero) for r in range(0, count, 16)], 0)


def store_halves(ref_hi, ref_lo, at, cols, value):
    hi, lo = halves(jnp.concatenate([value, jnp.zeros((PAD - FACE, value.shape[1]), F32)], 0))
    ref_hi[at : at + PAD, cols] = hi
    ref_lo[at : at + PAD, cols] = lo


def turned(packed, code, turn_t, stack_hi, stack_lo):
    hi = packed.astype(BF).astype(F32)
    lo = packed - hi
    for c in range(8):
        stack_hi[c * PAD : (c + 1) * PAD, :] = jnp.where(code == c, hi, 0.0).astype(BF)
        stack_lo[c * PAD : (c + 1) * PAD, :] = jnp.where(code == c, lo, 0.0).astype(BF)
    return dot(turn_t[...], stack_hi[...]) + dot(turn_t[...], stack_lo[...])


def tile_cols(t):
    return slice(t * LANES, (t + 1) * LANES)


def neighbour_index(rows, slot_v):
    elems = slot_v.shape[1]
    own = one_hot(slot_v[...], elems)
    base = 256.0
    table = jnp.concatenate(rows + [jnp.zeros((8 - len(rows), elems), F32)], 0)
    upper = jnp.floor(table * (1.0 / base))
    lower = table - upper * base
    both = jnp.concatenate([upper, lower], 0).astype(BF)
    moved = dot_t(both, own)
    return (moved[0:8] * base + moved[8:16]).astype(jnp.int32)


def first_kernel(
    per_span, axial, sectors, slot_l, turn_l, offset_l, slot_h, fields, velocity, sound, turn_h, forward_h,
    staged, th_a, iface, slot_v, plan, own_packed, forward_t, theta, turn_t, rows_hi, rows_lo, stack_hi, stack_lo, slot_s, turn_s, offset_s,
    sems, small_sems, out_sem,
):
    elems = slot_v.shape[1]
    tiles = elems // LANES
    half = axial // 2
    rows = VALS * PAD
    small = [
        pltpu.make_async_copy(slot_h, slot_v, small_sems.at[0]),
        pltpu.make_async_copy(turn_h, turn_t, small_sems.at[1]),
        pltpu.make_async_copy(slot_l, slot_s, small_sems.at[2]),
        pltpu.make_async_copy(turn_l, turn_s, small_sems.at[3]),
        pltpu.make_async_copy(offset_l, offset_s, small_sems.at[4]),
        pltpu.make_async_copy(forward_h, forward_t, small_sems.at[5]),
    ]
    loads = []
    for t in range(tiles):
        cols = pl.ds(t * LANES, LANES)
        loads.append([
            pltpu.make_async_copy(fields.at[:, :, cols], staged.at[0:5, t, 0:VOL, :], sems.at[t, 0]),
            pltpu.make_async_copy(velocity.at[:, :, cols], staged.at[5:8, t, 0:VOL, :], sems.at[t, 1]),
            pltpu.make_async_copy(sound.at[:, cols], staged.at[8, t, 0:VOL, :], sems.at[t, 2]),
        ])
        for copy in loads[-1]:
            copy.start()
    for copy in small:
        copy.start()
    for copy in small:
        copy.wait()
    sector = lax.axis_index("blk")
    lane = lane_iota((1, LANES))
    column = lane % (2 * per_span)
    target = jnp.full((1, LANES), -1, jnp.int32)
    code = jnp.zeros((1, LANES), jnp.int32)
    want = jnp.zeros((1, LANES), jnp.int32)
    forward = jnp.zeros((1, LANES), jnp.int32)
    for s in range(per_span):
        target = jnp.where(lane == s, slot_s[s * axial + half - 1], target)
        target = jnp.where(lane == per_span + s, slot_s[s * axial + half], target)
        code = jnp.where(column == per_span + s, turn_s[0, s], code)
        forward = jnp.where(column == s, turn_s[0, s], forward)
        shift = lax.rem(offset_s[s], sectors)
        want = jnp.where(column == s, lax.rem(sector - shift + sectors, sectors), want)
        want = jnp.where(column == per_span + s, lax.rem(sector + shift, sectors), want)
    plan[0:1, :] = want
    plan[1:2, :] = forward
    one = one_hot(target, elems)
    theta[VALS * FACE : VALS * FACE + 1, :] = jnp.zeros((1, elems), F32)
    odd = axis_parity("blk")

    for t in range(tiles):
        for copy in loads[t]:
            copy.wait()
        cols = tile_cols(t)

        @pl.when(odd == 0)
        def _():
            for f in range(VALS):
                theta[f * FACE : (f + 1) * FACE, cols] = face_rows(staged, value_index(f, 0), t, 0, ORDER)

        @pl.when(odd == 1)
        def _():
            for f in range(VALS):
                theta[f * FACE : (f + 1) * FACE, cols] = face_rows(staged, value_index(f, 0), t, 0, 0)

        for n, end in enumerate((ORDER, 0)):
            for f in range(VALS):
                at = n * rows + f * PAD
                store_halves(rows_hi, rows_lo, at, cols, face_rows(staged, value_index(f, 2), t, 2, end))
    out = pltpu.make_async_copy(theta, th_a, out_sem)
    out.start()
    both = dot(rows_hi[...], one) + dot(rows_lo[...], one)
    both = jnp.where(lane < per_span, both[0:rows], jnp.where(lane < 2 * per_span, both[rows:], 0.0))
    packed = both[0:PAD]
    for f in range(1, VALS):
        packed = packed + pltpu.roll(both[f * PAD : (f + 1) * PAD], f * 2 * per_span, 1)
    own_packed[...] = packed
    iface[...] = turned(packed, code, turn_t, stack_hi, stack_lo)
    for t in range(tiles):
        iface[PAD - tiles + t : PAD - tiles + t + 1, :] = slot_v[:, tile_cols(t)].astype(F32)
    out.wait()


LOCAL_FACES = ((1, 1), (1, 0), (2, 1), (2, 0))


def second_kernel(
    per_span, axial, slot_v, staged, th_b, sp_a, sp_b, index, rows_hi, rows_lo, theta, out_sem,
):
    elems = slot_v.shape[1]
    tiles = elems // LANES
    half = axial // 2
    rows = VALS * PAD
    theta[VALS * FACE : VALS * FACE + 1, :] = jnp.zeros((1, elems), F32)
    odd = axis_parity("blk")

    @pl.when(odd == 0)
    def _():
        for t in range(tiles):
            for f in range(VALS):
                theta[f * FACE : (f + 1) * FACE, tile_cols(t)] = face_rows(staged, value_index(f, 0), t, 0, 0)

    @pl.when(odd == 1)
    def _():
        for t in range(tiles):
            for f in range(VALS):
                theta[f * FACE : (f + 1) * FACE, tile_cols(t)] = face_rows(staged, value_index(f, 0), t, 0, ORDER)

    out = pltpu.make_async_copy(theta, th_b, out_sem)
    out.start()
    for n, (d, end) in enumerate(LOCAL_FACES):
        for t in range(tiles):
            for f in range(VALS):
                x = face_rows(staged, value_index(f, d), t, d, end * ORDER)
                store_halves(rows_hi, rows_lo, n * rows + f * PAD, tile_cols(t), x)

    def gathered(start, row):
        one = one_hot(row, elems)
        return dot(rows_hi[start : start + rows, :], one) + dot(rows_lo[start : start + rows, :], one)

    high = gathered(0, slot_v[:, elems - axial : elems])
    low = gathered(rows, slot_v[:, 0:axial])
    span_odd = axis_parity("span")

    @pl.when(span_odd == 0)
    def _():
        sp_a[...] = high
        sp_b[...] = low

    @pl.when(span_odd == 1)
    def _():
        sp_a[...] = low
        sp_b[...] = high

    slots = slot_v[...].astype(F32)
    lane = lane_iota((1, elems))
    position = lane % axial
    row = (lane // axial).astype(F32)
    lanes_f = lane.astype(F32)
    span_low = jnp.where(lane < axial, elems + lanes_f, pltpu.roll(slots, axial, 1))
    span_high = jnp.where(lane >= elems - axial, axial + lanes_f, pltpu.roll(slots, elems - axial, 1))
    none = elems + LANES - 1.0
    ax_low = jnp.where(position == half, elems + row, pltpu.roll(slots, 1, 1))
    ax_low = jnp.where(position == 0, none, ax_low)
    ax_high = jnp.where(position == half - 1, elems + per_span + row, pltpu.roll(slots, elems - 1, 1))
    ax_high = jnp.where(position == axial - 1, none, ax_high)
    index[...] = neighbour_index([span_low, span_high, ax_low, ax_high], slot_v)
    out.wait()


def local_kernel(index, rows_hi, rows_lo, ghosts):
    elems = index.shape[1]
    rows = VALS * PAD
    for n in range(len(LOCAL_FACES)):
        one = one_hot(index[n : n + 1, :], elems)
        at = slice(n * rows, (n + 1) * rows)
        ghosts[n] = dot(rows_hi[at, :], one) + dot(rows_lo[at, :], one)


def work_kernel(place, per_span, staged, index, ghosts, matrix_h, store_h, earlier, out, store, sems, *scratch):
    del earlier

    @pl.when(work_place() == place)
    def _():
        tiles = staged.shape[1]
        elems = tiles * LANES
        stores = [
            pltpu.make_async_copy(store_h.at[:, :, pl.ds(t * LANES, LANES)], store.at[:, t, 0:VOL, :], sems.at[t])
            for t in range(tiles)
        ]
        for copy in stores:
            copy.start()
        volume_terms(staged, matrix_h, out, *scratch)
        for copy in stores:
            copy.wait()
        for t in range(tiles):
            for f in range(5):
                out[f, t, 0:VOL, :] += section_decay * store[f, t, 0:VOL, :]
            for n, side in ((2, -1), (3, 1)):
                at = index[n : n + 1, tile_cols(t)]
                keep = jnp.logical_or(at < elems, at >= elems + 2 * per_span)
                side_terms(staged, ghosts.at[n], out, 2, side, t, keep=keep)


def work_start(place, per_span, staged, index, ghosts, matrix_h, store_h, out, *scratch):
    work_kernel(place, per_span, staged, index, ghosts, matrix_h, store_h, None, out, *scratch)


def work_place():
    return jnp.where(axis_parity("span") == 1, 0, 1)


def volume_terms(staged, matrix_h, out, matrix, flux_hi, flux_lo, sem):
    tiles = staged.shape[1]
    load = pltpu.make_async_copy(matrix_h, matrix, sem)
    load.start()
    step = 16
    for pair in range(tiles // 2):
        for half in range(2):
            t = 2 * pair + half
            cols = tile_cols(half)
            for r in range(0, VOL, step):
                n = min(step, VOL - r)
                rows = slice(r, r + n)
                q = [staged[f, t, rows, :] for f in range(5)]
                c = staged[8, t, rows, :]
                cp = c * q[4]
                for d in range(3):
                    m = staged[5 + d, t, rows, :]
                    cu = c * q[1 + d]
                    for f in range(5):
                        x = m * q[f]
                        if f in (0, 4):
                            x = x + cu
                        elif f == 1 + d:
                            x = x + cp
                        if n < step:
                            x = jnp.concatenate([x, jnp.zeros((step - n, LANES), F32)], 0)
                        hi, lo = halves(x)
                        flux_hi[pair, f, d * LANES + r : d * LANES + r + step, cols] = hi
                        flux_lo[pair, f, d * LANES + r : d * LANES + r + step, cols] = lo
        if pair == 0:
            load.wait()
        for f in range(5):
            a = dot(matrix[...], flux_hi[pair, f])
            b = dot(matrix[0:LANES, :], flux_lo[pair, f])
            total = a[0:LANES] + a[LANES : 2 * LANES] + b
            for half in range(2):
                out[f, 2 * pair + half] = total[:, tile_cols(half)]


def theta_ghost(recv, index_row):
    one = one_hot(index_row, recv.shape[1])
    hi, lo = halves(recv[...])
    return dot(hi, one) + dot(lo, one)


def theta_side(staged, ghost, acc, shift, side, t):
    start = ORDER * FACE if side > 0 else 0
    own = [staged[value_index(f, 0), t, start : start + FACE, :] for f in range(VALS)]
    other = [ghost[f * FACE : (f + 1) * FACE, tile_cols(t)] for f in range(VALS)]
    for f, x in enumerate(surface(own, other, 0, side)):
        acc[f, t, start - shift : start - shift + FACE, :] += x


HIGH_ROW = (ORDER * FACE) // PAD * PAD


def side_terms(staged, ghost_ref, acc, d, side, t, keep=None, wall=None):
    cols = tile_cols(t)
    end = ORDER if side > 0 else 0
    own = [face_rows(staged, value_index(f, d), t, d, end) for f in range(VALS)]
    other = [ghost_ref[f * PAD : f * PAD + FACE, cols] for f in range(VALS)]
    if wall is not None:
        for f in range(VALS):
            other[f] = jnp.where(wall, -own[f] if f == 1 + d else own[f], other[f])
    for f, x in enumerate(surface(own, other, d, side)):
        add_face_rows(acc, f, t, d, end, x if keep is None else jnp.where(keep, x, 0.0))


def face_kernel(slot_v, staged, index, ghosts, th_a, sp_a, iface_a, part, acc, ghost, whole):
    del part
    tiles = staged.shape[1]
    odd = axis_parity("blk")
    slots_a = jnp.concatenate([iface_a[PAD - tiles + t : PAD - tiles + t + 1, :] for t in range(tiles)], 1)
    ghost[...] = theta_ghost(th_a, neighbour_index([slots_a], slot_v)[0:1])
    span_side(0, staged, index, ghosts, sp_a, acc, whole, None)
    for t in range(tiles):
        @pl.when(odd == 0)
        def _():
            theta_side(staged, ghost, acc, 0, 1, t)

        @pl.when(odd == 1)
        def _():
            theta_side(staged, ghost, acc, 0, -1, t)


def span_side(other_pair, staged, index, ghosts, received, acc, whole, wall, tile=None):
    slab_odd = axis_parity("span")
    for n, side in ((0, -1), (1, 1)):
        @pl.when(slab_odd == (1 - n if other_pair == 0 else n))
        def _():
            elems = index.shape[1]
            if tile in (None, 0):
                hi, lo = halves(received[...])
                one = one_hot(index[n : n + 1, :] - elems, LANES)
                whole[...] = ghosts[n] + (dot(hi, one) + dot(lo, one))
            for t in range(staged.shape[1]) if tile is None else (tile,):
                at_wall = None
                if wall is not None:
                    at_wall = jnp.logical_and(index[n : n + 1, tile_cols(t)] >= elems, wall)
                side_terms(staged, whole, acc, 1, side, t, wall=at_wall)


def late_kernel(
    per_span, sectors, slabs, pieces, far,
    plan, slot_v, staged, index, ghosts, own_packed, sp_b, turn_t, part, *rest,
):
    del part
    iface = rest[:pieces]
    fields_out, store_out, acc, index_b = rest[pieces : pieces + 4]
    fresh, whole, stack_hi, stack_lo, sems = rest[pieces + 4 :]
    elems = slot_v.shape[1]
    tiles = elems // LANES
    sector = lax.axis_index("blk")
    odd = lax.rem(sector, 2)

    partner = lax.rem(sector + jnp.where(odd == 1, 1, sectors - 1), sectors)
    slots_b = jnp.zeros((tiles, LANES), F32)
    want, code = plan[0:1, :], plan[1:2, :]
    near = jnp.zeros((PAD, LANES), F32)
    blocks = [piece[b * PAD : (b + 1) * PAD, :] for piece in iface for b in range(piece.shape[0] // PAD)]
    for k, block in zip(far, blocks):
        near = jnp.where(want == (sector ^ k), block, near)
        slots_b = jnp.where(partner == (sector ^ k), block[PAD - tiles :], slots_b)
    flat = lambda x: jnp.concatenate([x[t : t + 1] for t in range(tiles)], 1)
    index_b[...] = neighbour_index([flat(slots_b)], slot_v)
    slab = lax.axis_index("span")

    near = turned(near, code, turn_t, stack_hi, stack_lo)
    lane = lane_iota((1, LANES))
    used = lane < 2 * per_span
    own, other = [], []
    for f in range(VALS):
        at = f * 2 * per_span
        down = pltpu.roll(own_packed[...], LANES - at - per_span, 1)
        up = pltpu.roll(own_packed[...], (LANES - at + per_span) % LANES, 1)
        own.append(jnp.where(used, jnp.where(lane < per_span, down, up), 0.0))
        theirs = near if f == 0 else pltpu.roll(near, LANES - at, 1)
        other.append(jnp.where(used, theirs, 0.0))
    low = surface(own, other, 2, -1)
    high = surface(own, other, 2, 1)
    terms = jnp.concatenate([jnp.where(lane < per_span, x, y) for x, y in zip(low, high)], 0)
    hi, lo = halves(jnp.where(used, terms, 0.0))

    def placed(n):
        one = one_hot(index[n : n + 1, :] - elems, LANES)
        return dot(hi, one) + dot(lo, one)

    fixes = (placed(2), placed(3))

    def copies(t, low_row, high_row):
        cols = pl.ds(t * LANES, LANES)
        rows = slice(low_row, high_row)
        return (
            pltpu.make_async_copy(acc.at[:, t, rows, :], store_out.at[:, rows, cols], sems.at[t, 0]),
            pltpu.make_async_copy(fresh.at[:, t, rows, :], fields_out.at[:, rows, cols], sems.at[t, 1]),
        )

    def each_way(action):
        @pl.when(odd == 0)
        def _():
            action(PAD, VOL)

        @pl.when(odd == 1)
        def _():
            action(0, HIGH_ROW)

    def send(t):
        def action(low_row, high_row):
            for copy in copies(t, low_row, high_row):
                copy.start()

        return action

    def wait(low_row, high_row):
        for t in range(tiles):
            for copy in copies(t, low_row, high_row):
                copy.wait()

    for t in range(tiles):
        span_side(1, staged, index, ghosts, sp_b, acc, whole, jnp.logical_or(slab == 0, slab == slabs - 1), t)
        for f in range(5):
            for fix, end in zip(fixes, (0, ORDER)):
                add_face_rows(acc, f, t, 2, end, fix[f * PAD : f * PAD + FACE, tile_cols(t)])
        for f in range(5):
            fresh[f, t, 0:VOL, :] = staged[f, t, 0:VOL, :] + section_gain * acc[f, t, 0:VOL, :]
        each_way(send(t))
    each_way(wait)


def last_kernel(index_b, staged, part, th_b, fields_in, store_in, fields_out, store_out, ghost, acc, fresh, sems):
    del fields_in, store_in
    tiles = staged.shape[1]
    ghost[...] = theta_ghost(th_b, index_b[0:1])

    def finish(side, low, high):
        copies = []
        for t in range(tiles):
            for f in range(5):
                acc[f, t, 0 : high - low, :] = part[f, t, low:high, :]
            theta_side(staged, ghost, acc, low, side, t)
            for f in range(5):
                fresh[f, t, 0 : high - low, :] = (
                    staged[f, t, low:high, :] + section_gain * acc[f, t, 0 : high - low, :]
                )
            cols = pl.ds(t * LANES, LANES)
            pair = (
                pltpu.make_async_copy(acc.at[:, t, 0 : high - low, :], store_out.at[:, low:high, cols], sems.at[t, 0]),
                pltpu.make_async_copy(fresh.at[:, t, 0 : high - low, :], fields_out.at[:, low:high, cols], sems.at[t, 1]),
            )
            for copy in pair:
                copy.start()
            copies.extend(pair)
        for copy in copies:
            copy.wait()

    odd = axis_parity("blk")

    @pl.when(odd == 0)
    def _():
        finish(-1, 0, PAD)

    @pl.when(odd == 1)
    def _():
        finish(1, HIGH_ROW, VOL)


def params(limit=VMEM_LIMIT):
    return pltpu.CompilerParams(vmem_limit_bytes=limit)


def vmem_spec():
    return pl.BlockSpec(memory_space=pltpu.VMEM)


def hbm_spec():
    return pl.BlockSpec(memory_space=pltpu.HBM)


def in_hbm(x):
    return pltpu.with_memory_space_constraint(x, pltpu.HBM)


def in_vmem(x):
    return pltpu.with_memory_space_constraint(x, pltpu.VMEM)


def reaches(sectors):
    steps = [1 << bit for bit in range(sectors.bit_length() - 1)]
    return steps[:1] + steps[:0:-1]


def on_device(fields, section_store, mean_velocity, sound_speed, element_slot, face_turn, rotor_offset):
    per_theta, per_span = face_turn.shape
    elems = element_slot.shape[0]
    axial = elems // (per_theta * per_span)
    sectors, slabs = lax.axis_size("blk"), lax.axis_size("span")
    tiles = elems // LANES
    rows = VALS * PAD
    assert per_theta == 1 and axial == LANES and sectors % 2 == 0 and sectors & (sectors - 1) == 0
    assert 2 * per_span * VALS < LANES and FACE + tiles <= PAD
    dma = pltpu.SemaphoreType.DMA
    theta_rows = VALS * FACE + 1
    vmem, hbm = pltpu.VMEM, pltpu.HBM
    slot_h = in_hbm(element_slot.reshape(1, elems))
    stack = [vmem((8 * PAD, LANES), BF), vmem((8 * PAD, LANES), BF)]
    staged, th_a, iface, slot_v, plan, own_packed, forward_t = pl.pallas_call(
        functools.partial(first_kernel, per_span, axial, sectors),
        out_shape=(
            vmem((9, tiles, LANES, LANES), F32),
            hbm((theta_rows, elems), F32),
            vmem((PAD, LANES), F32),
            vmem((1, elems), jnp.int32),
            vmem((8, LANES), jnp.int32),
            vmem((PAD, LANES), F32),
            vmem((PAD, 8 * PAD), BF),
        ),
        in_specs=[hbm_spec()] * 9,
        out_specs=(vmem_spec(), hbm_spec()) + (vmem_spec(),) * 5,
        scratch_shapes=[
            vmem((theta_rows, elems), F32),
            vmem((PAD, 8 * PAD), BF),
            vmem((2 * rows, elems), BF),
            vmem((2 * rows, elems), BF),
            *stack,
            pltpu.SMEM((elems,), jnp.int32),
            pltpu.SMEM((per_theta, per_span), jnp.int32),
            pltpu.SMEM((per_span,), jnp.int32),
            dma((tiles, 3)),
            dma((6,)),
            dma(()),
        ],
        compiler_params=params(),
        name="first",
    )(
        in_hbm(element_slot), in_hbm(face_turn), in_hbm(rotor_offset), slot_h, in_hbm(fields), in_hbm(mean_velocity), in_hbm(sound_speed),
        in_hbm(jnp.asarray(turn_matrix(True))), in_hbm(jnp.asarray(turn_matrix(False))),
    )

    pieces, far = [iface], [0]
    near_a = lax.ppermute(th_a, "blk", [(i, i ^ 1) for i in range(sectors)])
    for reach in reaches(sectors):
        block = jnp.concatenate(pieces, 0)
        pieces.append(lax.ppermute(block, "blk", [(i, i ^ reach) for i in range(sectors)]))
        far += [k ^ reach for k in far]

    th_b, sp_a, sp_b, index, rows_hi, rows_lo = pl.pallas_call(
        functools.partial(second_kernel, per_span, axial),
        out_shape=(
            hbm((theta_rows, elems), F32),
            vmem((rows, LANES), F32),
            vmem((rows, LANES), F32),
            vmem((8, elems), jnp.int32),
            vmem((len(LOCAL_FACES) * rows, elems), BF),
            vmem((len(LOCAL_FACES) * rows, elems), BF),
        ),
        in_specs=[vmem_spec()] * 2,
        out_specs=(hbm_spec(),) + (vmem_spec(),) * 5,
        scratch_shapes=[vmem((theta_rows, elems), F32), dma(())],
        compiler_params=params(),
        name="second",
    )(in_vmem(slot_v), in_vmem(staged))
    pairs = [(i, (i + 1 if i % 2 else i - 1) % sectors) for i in range(sectors)]
    near_b = lax.ppermute(th_b, "blk", pairs)
    span_a = lax.ppermute(sp_a, "span", [(i, i ^ 1) for i in range(slabs) if i ^ 1 < slabs])
    pairs = [(i, i + 1 if i % 2 else i - 1) for i in range(slabs)]
    span_b = lax.ppermute(sp_b, "span", [(i, j) for i, j in pairs if 0 <= j < slabs])

    ghosts = pl.pallas_call(
        local_kernel,
        out_shape=vmem((len(LOCAL_FACES), rows, elems), F32),
        in_specs=[vmem_spec()] * 3,
        out_specs=vmem_spec(),
        compiler_params=params(),
        name="local",
    )(in_vmem(index), in_vmem(rows_hi), in_vmem(rows_lo))

    part = None
    block = (5, tiles, LANES, LANES)
    for place in range(2):
        work = pl.pallas_call(
            functools.partial(work_kernel if place else work_start, place, per_span),
            out_shape=vmem(block, F32),
            in_specs=[vmem_spec()] * 3 + [hbm_spec()] * 2 + [vmem_spec()] * (place > 0),
            out_specs=vmem_spec(),
            scratch_shapes=[
                vmem(block, F32),
                dma((tiles,)),
                vmem((2 * LANES, 3 * LANES), BF),
                vmem((tiles // 2, 5, 3 * LANES, 2 * LANES), BF),
                vmem((tiles // 2, 5, 3 * LANES, 2 * LANES), BF),
                dma(()),
            ],
            input_output_aliases={5: 0} if place else {},
            compiler_params=params(),
        )
        operands = [in_vmem(staged), in_vmem(index), in_vmem(ghosts)]
        operands += [in_hbm(jnp.asarray(volume_matrix())), in_hbm(section_store)]
        if place:
            operands.append(in_vmem(part))
        part = work(*operands)

    part = pl.pallas_call(
        face_kernel,
        out_shape=vmem(block, F32),
        in_specs=[vmem_spec()] * 8,
        out_specs=vmem_spec(),
        scratch_shapes=[vmem((theta_rows, elems), F32), vmem((rows, elems), F32)],
        input_output_aliases={7: 0},
        compiler_params=params(),
        name="faces",
    )(
        in_vmem(slot_v), in_vmem(staged), in_vmem(index), in_vmem(ghosts), in_vmem(near_a), in_vmem(span_a),
        in_vmem(pieces[1]), in_vmem(part),
    )

    whole = hbm((5, VOL, elems), F32)
    fields_part, store_part, part, index_b = pl.pallas_call(
        functools.partial(late_kernel, per_span, sectors, slabs, len(pieces), far),
        out_shape=(whole, whole, vmem(block, F32), vmem((8, elems), jnp.int32)),
        in_specs=[vmem_spec()] * (9 + len(pieces)),
        out_specs=(hbm_spec(),) * 2 + (vmem_spec(),) * 2,
        scratch_shapes=[
            vmem(block, F32),
            vmem((rows, elems), F32),
            *stack,
            dma((tiles, 2)),
        ],
        input_output_aliases={8: 2},
        compiler_params=params(),
        name="late",
    )(
        in_vmem(plan), in_vmem(slot_v), in_vmem(staged), in_vmem(index), in_vmem(ghosts), in_vmem(own_packed),
        in_vmem(span_b), in_vmem(forward_t), in_vmem(part), *[in_vmem(piece) for piece in pieces],
    )

    return pl.pallas_call(
        last_kernel,
        out_shape=(whole, whole),
        in_specs=[vmem_spec()] * 4 + [hbm_spec()] * 2,
        out_specs=(hbm_spec(),) * 2,
        scratch_shapes=[
            vmem((theta_rows, elems), F32),
            vmem((5, tiles, PAD, LANES), F32),
            vmem((5, tiles, PAD, LANES), F32),
            dma((tiles, 2)),
        ],
        input_output_aliases={4: 0, 5: 1},
        compiler_params=params(),
        name="last",
    )(in_vmem(index_b), in_vmem(staged), in_vmem(part), in_vmem(near_b), fields_part, store_part)


def solution(mesh):
    both = ("blk", "span")
    in_specs = (
        P(None, None, both),
        P(None, None, both),
        P(None, None, both),
        P(None, both),
        P(both),
        P("blk", "span"),
        P("span"),
    )
    out_specs = (P(None, None, both), P(None, None, both))
    return jax.shard_map(on_device, mesh=mesh, in_specs=in_specs, out_specs=out_specs, check_vma=False)
```

```python
import functools

import jax
import jax.numpy as jnp
import numpy as np
from jax import lax
from jax.experimental import pallas as pl
from jax.experimental.pallas import tpu as pltpu
from jax.sharding import PartitionSpec as P


ORDER = 4
NODE = ORDER + 1
FACE = NODE * NODE
VOL = NODE**3
LANES = 128
PAD = 32
VALS = 7

section_decay = -567301805773.0 / 1357537059087.0
section_gain = 5161836677717.0 / 13612068292357.0
time_step = 0.05
metric_scale = (1.0, 1.5, 0.75)
end_weight = 0.1

BF = jnp.bfloat16
F32 = jnp.float32
VMEM_LIMIT = 24 * 1024 * 1024


def lobatto_slopes():
    inner_root = np.sqrt(3.0 / 7.0)
    points = np.array([-1.0, -inner_root, 0.0, inner_root, 1.0])
    count = points.shape[0]
    slopes = np.zeros((count, count))
    for r in range(count):
        for c in range(count):
            if r == c:
                slopes[r, c] = sum(1.0 / (points[r] - points[o]) for o in range(count) if o != r)
            else:
                top = np.prod([points[r] - points[o] for o in range(count) if o != r])
                low = np.prod([points[c] - points[o] for o in range(count) if o != c])
                slopes[r, c] = top / (low * (points[r] - points[c]))
    return slopes


def split_np(table):
    high = np.asarray(table, np.float32).astype(BF)
    low = (np.asarray(table, np.float64) - high.astype(np.float64)).astype(BF)
    return high, low


def volume_matrix():
    slopes = lobatto_slopes()
    eye = np.eye(NODE)
    parts = (
        np.kron(np.kron(slopes, eye), eye),
        np.kron(np.kron(eye, slopes), eye),
        np.kron(np.kron(eye, eye), slopes),
    )
    full = np.zeros((LANES, 3 * LANES))
    for d in range(3):
        full[:VOL, d * LANES : d * LANES + VOL] = -time_step * metric_scale[d] * parts[d]
    high, low = split_np(full)
    return np.concatenate([high, low], 0)


def turn_matrix(inverse):
    table = np.zeros((PAD, 8 * PAD), np.float32)
    for code in range(8):
        index = np.arange(FACE).reshape(NODE, NODE)
        if inverse:
            if code & 2:
                index = index[:, ::-1]
            if code & 1:
                index = index[::-1, :]
            if code & 4:
                index = index.T
        else:
            if code & 4:
                index = index.T
            if code & 1:
                index = index[::-1, :]
            if code & 2:
                index = index[:, ::-1]
        for n, o in enumerate(index.reshape(-1)):
            table[n, code * PAD + o] = 1.0
    return table.astype(BF)


def dot(a, b):
    return jnp.dot(a, b, preferred_element_type=F32)


def dot_t(a, b):
    return lax.dot_general(a, b, (((1,), (1,)), ((), ())), preferred_element_type=F32)


def halves(x):
    high = x.astype(BF)
    return high, (x - high.astype(F32)).astype(BF)


def lane_iota(shape):
    return lax.broadcasted_iota(jnp.int32, shape, len(shape) - 1)


def face_rows(ref, v, tile, d, end):
    if d == 0:
        return ref[v, tile, pl.ds(end * FACE, FACE), :]
    if d == 1:
        starts = [i * FACE + end * NODE for i in range(NODE)]
        return jnp.concatenate([ref[v, tile, pl.ds(s, NODE), :] for s in starts], axis=0)
    return ref[v, tile, pl.ds(end, FACE, NODE), :]


def add_face_rows(ref, v, tile, d, end, value):
    if d == 0:
        ref[v, tile, pl.ds(end * FACE, FACE), :] += value
    elif d == 1:
        for i in range(NODE):
            ref[v, tile, pl.ds(i * FACE + end * NODE, NODE), :] += value[i * NODE : (i + 1) * NODE]
    else:
        ref[v, tile, pl.ds(end, FACE, NODE), :] += value


def value_index(f, d):
    return f if f < 5 else (5 + d if f == 5 else 8)


def surface(own, other, d, side):
    qo, mo, co = own[:5], own[5], own[6]
    qn, mn, cn = other[:5], other[5], other[6]
    reach = jnp.maximum(jnp.abs(mo) + co, jnp.abs(mn) + cn)
    weight = side * 0.5 * time_step * metric_scale[d] / end_weight
    if side > 0:
        ao, an = mo - reach, mn - reach
    else:
        ao, an = mo + reach, mn + reach
    velocity_part = co * qo[1 + d] - cn * qn[1 + d]
    pressure_part = co * qo[4] - cn * qn[4]
    out = []
    for f in range(5):
        x = ao * qo[f] - an * qn[f]
        if f in (0, 4):
            x = x + velocity_part
        elif f == 1 + d:
            x = x + pressure_part
        out.append(weight * x)
    return out


def axis_parity(axis):
    return lax.rem(lax.axis_index(axis), 2)


def one_hot(index_row, count):
    short = jnp.broadcast_to(index_row, (16, index_row.shape[1])).astype(jnp.int16)
    rows = lax.broadcasted_iota(jnp.int16, (16, index_row.shape[1]), 0)
    one, zero = jnp.ones(short.shape, BF), jnp.zeros(short.shape, BF)
    return jnp.concatenate([jnp.where(rows == short - r, one, zero) for r in range(0, count, 16)], 0)


def store_halves(ref_hi, ref_lo, at, cols, value):
    hi, lo = halves(jnp.concatenate([value, jnp.zeros((PAD - FACE, value.shape[1]), F32)], 0))
    ref_hi[at : at + PAD, cols] = hi
    ref_lo[at : at + PAD, cols] = lo


def turned(packed, code, turn_t, stack_hi, stack_lo):
    hi = packed.astype(BF).astype(F32)
    lo = packed - hi
    for c in range(8):
        stack_hi[c * PAD : (c + 1) * PAD, :] = jnp.where(code == c, hi, 0.0).astype(BF)
        stack_lo[c * PAD : (c + 1) * PAD, :] = jnp.where(code == c, lo, 0.0).astype(BF)
    return dot(turn_t[...], stack_hi[...]) + dot(turn_t[...], stack_lo[...])


def tile_cols(t):
    return slice(t * LANES, (t + 1) * LANES)


def neighbour_index(rows, slot_v):
    elems = slot_v.shape[1]
    own = one_hot(slot_v[...], elems)
    base = 256.0
    table = jnp.concatenate(rows + [jnp.zeros((8 - len(rows), elems), F32)], 0)
    upper = jnp.floor(table * (1.0 / base))
    lower = table - upper * base
    both = jnp.concatenate([upper, lower], 0).astype(BF)
    moved = dot_t(both, own)
    return (moved[0:8] * base + moved[8:16]).astype(jnp.int32)


def first_kernel(
    per_span, axial, sectors, slot_l, turn_l, offset_l, slot_h, fields, velocity, sound, turn_h, forward_h,
    staged, th_a, iface, slot_v, plan, own_packed, forward_t, theta, turn_t, rows_hi, rows_lo, stack_hi, stack_lo, slot_s, turn_s, offset_s,
    sems, small_sems, out_sem,
):
    elems = slot_v.shape[1]
    tiles = elems // LANES
    half = axial // 2
    rows = VALS * PAD
    small = [
        pltpu.make_async_copy(slot_h, slot_v, small_sems.at[0]),
        pltpu.make_async_copy(turn_h, turn_t, small_sems.at[1]),
        pltpu.make_async_copy(slot_l, slot_s, small_sems.at[2]),
        pltpu.make_async_copy(turn_l, turn_s, small_sems.at[3]),
        pltpu.make_async_copy(offset_l, offset_s, small_sems.at[4]),
        pltpu.make_async_copy(forward_h, forward_t, small_sems.at[5]),
    ]
    loads = []
    for t in range(tiles):
        cols = pl.ds(t * LANES, LANES)
        loads.append([
            pltpu.make_async_copy(fields.at[:, :, cols], staged.at[0:5, t, 0:VOL, :], sems.at[t, 0]),
            pltpu.make_async_copy(velocity.at[:, :, cols], staged.at[5:8, t, 0:VOL, :], sems.at[t, 1]),
            pltpu.make_async_copy(sound.at[:, cols], staged.at[8, t, 0:VOL, :], sems.at[t, 2]),
        ])
        for copy in loads[-1]:
            copy.start()
    for copy in small:
        copy.start()
    for copy in small:
        copy.wait()
    sector = lax.axis_index("blk")
    lane = lane_iota((1, LANES))
    column = lane % (2 * per_span)
    target = jnp.full((1, LANES), -1, jnp.int32)
    code = jnp.zeros((1, LANES), jnp.int32)
    want = jnp.zeros((1, LANES), jnp.int32)
    forward = jnp.zeros((1, LANES), jnp.int32)
    for s in range(per_span):
        target = jnp.where(lane == s, slot_s[s * axial + half - 1], target)
        target = jnp.where(lane == per_span + s, slot_s[s * axial + half], target)
        code = jnp.where(column == per_span + s, turn_s[0, s], code)
        forward = jnp.where(column == s, turn_s[0, s], forward)
        shift = lax.rem(offset_s[s], sectors)
        want = jnp.where(column == s, lax.rem(sector - shift + sectors, sectors), want)
        want = jnp.where(column == per_span + s, lax.rem(sector + shift, sectors), want)
    plan[0:1, :] = want
    plan[1:2, :] = forward
    one = one_hot(target, elems)
    theta[VALS * FACE : VALS * FACE + 1, :] = jnp.zeros((1, elems), F32)
    odd = axis_parity("blk")

    for t in range(tiles):
        for copy in loads[t]:
            copy.wait()
        cols = tile_cols(t)

        @pl.when(odd == 0)
        def _():
            for f in range(VALS):
                theta[f * FACE : (f + 1) * FACE, cols] = face_rows(staged, value_index(f, 0), t, 0, ORDER)

        @pl.when(odd == 1)
        def _():
            for f in range(VALS):
                theta[f * FACE : (f + 1) * FACE, cols] = face_rows(staged, value_index(f, 0), t, 0, 0)

        for n, end in enumerate((ORDER, 0)):
            for f in range(VALS):
                at = n * rows + f * PAD
                store_halves(rows_hi, rows_lo, at, cols, face_rows(staged, value_index(f, 2), t, 2, end))
    out = pltpu.make_async_copy(theta, th_a, out_sem)
    out.start()
    both = dot(rows_hi[...], one) + dot(rows_lo[...], one)
    both = jnp.where(lane < per_span, both[0:rows], jnp.where(lane < 2 * per_span, both[rows:], 0.0))
    packed = both[0:PAD]
    for f in range(1, VALS):
        packed = packed + pltpu.roll(both[f * PAD : (f + 1) * PAD], f * 2 * per_span, 1)
    own_packed[...] = packed
    iface[...] = turned(packed, code, turn_t, stack_hi, stack_lo)
    for t in range(tiles):
        iface[PAD - tiles + t : PAD - tiles + t + 1, :] = slot_v[:, tile_cols(t)].astype(F32)
    out.wait()


LOCAL_FACES = ((1, 1), (1, 0), (2, 1), (2, 0))


def second_kernel(
    per_span, axial, slot_v, staged, th_b, sp_a, sp_b, index, rows_hi, rows_lo, theta, out_sem,
):
    elems = slot_v.shape[1]
    tiles = elems // LANES
    half = axial // 2
    rows = VALS * PAD
    theta[VALS * FACE : VALS * FACE + 1, :] = jnp.zeros((1, elems), F32)
    odd = axis_parity("blk")

    @pl.when(odd == 0)
    def _():
        for t in range(tiles):
            for f in range(VALS):
                theta[f * FACE : (f + 1) * FACE, tile_cols(t)] = face_rows(staged, value_index(f, 0), t, 0, 0)

    @pl.when(odd == 1)
    def _():
        for t in range(tiles):
            for f in range(VALS):
                theta[f * FACE : (f + 1) * FACE, tile_cols(t)] = face_rows(staged, value_index(f, 0), t, 0, ORDER)

    out = pltpu.make_async_copy(theta, th_b, out_sem)
    out.start()
    for n, (d, end) in enumerate(LOCAL_FACES):
        for t in range(tiles):
            for f in range(VALS):
                x = face_rows(staged, value_index(f, d), t, d, end * ORDER)
                store_halves(rows_hi, rows_lo, n * rows + f * PAD, tile_cols(t), x)

    def gathered(start, row):
        one = one_hot(row, elems)
        return dot(rows_hi[start : start + rows, :], one) + dot(rows_lo[start : start + rows, :], one)

    high = gathered(0, slot_v[:, elems - axial : elems])
    low = gathered(rows, slot_v[:, 0:axial])
    span_odd = axis_parity("span")

    @pl.when(span_odd == 0)
    def _():
        sp_a[...] = high
        sp_b[...] = low

    @pl.when(span_odd == 1)
    def _():
        sp_a[...] = low
        sp_b[...] = high

    slots = slot_v[...].astype(F32)
    lane = lane_iota((1, elems))
    position = lane % axial
    row = (lane // axial).astype(F32)
    lanes_f = lane.astype(F32)
    span_low = jnp.where(lane < axial, elems + lanes_f, pltpu.roll(slots, axial, 1))
    span_high = jnp.where(lane >= elems - axial, axial + lanes_f, pltpu.roll(slots, elems - axial, 1))
    none = elems + LANES - 1.0
    ax_low = jnp.where(position == half, elems + row, pltpu.roll(slots, 1, 1))
    ax_low = jnp.where(position == 0, none, ax_low)
    ax_high = jnp.where(position == half - 1, elems + per_span + row, pltpu.roll(slots, elems - 1, 1))
    ax_high = jnp.where(position == axial - 1, none, ax_high)
    index[...] = neighbour_index([span_low, span_high, ax_low, ax_high], slot_v)
    out.wait()


def local_kernel(index, rows_hi, rows_lo, ghosts):
    elems = index.shape[1]
    rows = VALS * PAD
    for n in range(len(LOCAL_FACES)):
        one = one_hot(index[n : n + 1, :], elems)
        at = slice(n * rows, (n + 1) * rows)
        ghosts[n] = dot(rows_hi[at, :], one) + dot(rows_lo[at, :], one)


def work_kernel(place, per_span, staged, index, ghosts, matrix_h, store_h, earlier, out, store, sems, *scratch):
    del earlier

    @pl.when(work_place() == place)
    def _():
        tiles = staged.shape[1]
        elems = tiles * LANES
        stores = [
            pltpu.make_async_copy(store_h.at[:, :, pl.ds(t * LANES, LANES)], store.at[:, t, 0:VOL, :], sems.at[t])
            for t in range(tiles)
        ]
        for copy in stores:
            copy.start()
        volume_terms(staged, matrix_h, out, *scratch)
        for copy in stores:
            copy.wait()
        for t in range(tiles):
            for f in range(5):
                out[f, t, 0:VOL, :] += section_decay * store[f, t, 0:VOL, :]
            for n, side in ((2, -1), (3, 1)):
                at = index[n : n + 1, tile_cols(t)]
                keep = jnp.logical_or(at < elems, at >= elems + 2 * per_span)
                side_terms(staged, ghosts.at[n], out, 2, side, t, keep=keep)


def work_start(place, per_span, staged, index, ghosts, matrix_h, store_h, out, *scratch):
    work_kernel(place, per_span, staged, index, ghosts, matrix_h, store_h, None, out, *scratch)


def work_place():
    return jnp.where(axis_parity("span") == 1, 0, 1)


def volume_terms(staged, matrix_h, out, matrix, flux_hi, flux_lo, sem):
    tiles = staged.shape[1]
    load = pltpu.make_async_copy(matrix_h, matrix, sem)
    load.start()
    step = 16
    for pair in range(tiles // 2):
        for half in range(2):
            t = 2 * pair + half
            cols = tile_cols(half)
            for r in range(0, VOL, step):
                n = min(step, VOL - r)
                rows = slice(r, r + n)
                q = [staged[f, t, rows, :] for f in range(5)]
                c = staged[8, t, rows, :]
                cp = c * q[4]
                for d in range(3):
                    m = staged[5 + d, t, rows, :]
                    cu = c * q[1 + d]
                    for f in range(5):
                        x = m * q[f]
                        if f in (0, 4):
                            x = x + cu
                        elif f == 1 + d:
                            x = x + cp
                        if n < step:
                            x = jnp.concatenate([x, jnp.zeros((step - n, LANES), F32)], 0)
                        hi, lo = halves(x)
                        flux_hi[pair, f, d * LANES + r : d * LANES + r + step, cols] = hi
                        flux_lo[pair, f, d * LANES + r : d * LANES + r + step, cols] = lo
        if pair == 0:
            load.wait()
        for f in range(5):
            a = dot(matrix[...], flux_hi[pair, f])
            b = dot(matrix[0:LANES, :], flux_lo[pair, f])
            total = a[0:LANES] + a[LANES : 2 * LANES] + b
            for half in range(2):
                out[f, 2 * pair + half] = total[:, tile_cols(half)]


def theta_ghost(recv, index_row):
    one = one_hot(index_row, recv.shape[1])
    hi, lo = halves(recv[...])
    return dot(hi, one) + dot(lo, one)


def theta_side(staged, ghost, acc, side, t):
    start = ORDER * FACE if side > 0 else 0
    own = [staged[value_index(f, 0), t, start : start + FACE, :] for f in range(VALS)]
    other = [ghost[f * FACE : (f + 1) * FACE, tile_cols(t)] for f in range(VALS)]
    for f, x in enumerate(surface(own, other, 0, side)):
        acc[f, t, start : start + FACE, :] += x


def side_terms(staged, ghost_ref, acc, d, side, t, keep=None, wall=None):
    cols = tile_cols(t)
    end = ORDER if side > 0 else 0
    own = [face_rows(staged, value_index(f, d), t, d, end) for f in range(VALS)]
    other = [ghost_ref[f * PAD : f * PAD + FACE, cols] for f in range(VALS)]
    if wall is not None:
        for f in range(VALS):
            other[f] = jnp.where(wall, -own[f] if f == 1 + d else own[f], other[f])
    for f, x in enumerate(surface(own, other, d, side)):
        add_face_rows(acc, f, t, d, end, x if keep is None else jnp.where(keep, x, 0.0))


def face_kernel(slot_v, staged, index, ghosts, th_a, sp_a, iface_a, part, acc, whole, ghost):
    del part
    tiles = staged.shape[1]
    odd = axis_parity("blk")
    slots_a = jnp.concatenate([iface_a[PAD - tiles + t : PAD - tiles + t + 1, :] for t in range(tiles)], 1)
    ghost[...] = theta_ghost(th_a, neighbour_index([slots_a], slot_v)[0:1])
    span_side(0, staged, index, ghosts, sp_a, acc, whole, None)
    for t in range(tiles):
        @pl.when(odd == 0)
        def _():
            theta_side(staged, ghost, acc, 1, t)

        @pl.when(odd == 1)
        def _():
            theta_side(staged, ghost, acc, -1, t)


def interface_kernel(
    per_span, sectors, pieces, far,
    plan, slot_v, index, own_packed, turn_t, part, *rest,
):
    del part
    iface = rest[:pieces]
    acc, picks, stack_hi, stack_lo = rest[pieces:]
    elems = slot_v.shape[1]
    tiles = elems // LANES
    sector = lax.axis_index("blk")
    odd = lax.rem(sector, 2)

    partner = lax.rem(sector + jnp.where(odd == 1, 1, sectors - 1), sectors)
    slots_b = jnp.zeros((tiles, LANES), F32)
    want, code = plan[0:1, :], plan[1:2, :]
    near = jnp.zeros((PAD, LANES), F32)
    blocks = [piece[b * PAD : (b + 1) * PAD, :] for piece in iface for b in range(piece.shape[0] // PAD)]
    for k, block in zip(far, blocks):
        near = jnp.where(want == (sector ^ k), block, near)
        slots_b = jnp.where(partner == (sector ^ k), block[PAD - tiles :], slots_b)
    flat = lambda x: jnp.concatenate([x[t : t + 1] for t in range(tiles)], 1)
    picks[...] = one_hot(neighbour_index([flat(slots_b)], slot_v)[0:1], elems)

    near = turned(near, code, turn_t, stack_hi, stack_lo)
    lane = lane_iota((1, LANES))
    used = lane < 2 * per_span
    own, other = [], []
    for f in range(VALS):
        at = f * 2 * per_span
        down = pltpu.roll(own_packed[...], LANES - at - per_span, 1)
        up = pltpu.roll(own_packed[...], (LANES - at + per_span) % LANES, 1)
        own.append(jnp.where(used, jnp.where(lane < per_span, down, up), 0.0))
        theirs = near if f == 0 else pltpu.roll(near, LANES - at, 1)
        other.append(jnp.where(used, theirs, 0.0))
    low = surface(own, other, 2, -1)
    high = surface(own, other, 2, 1)
    terms = jnp.concatenate([jnp.where(lane < per_span, x, y) for x, y in zip(low, high)], 0)
    hi, lo = halves(jnp.where(used, terms, 0.0))

    def placed(n):
        one = one_hot(index[n : n + 1, :] - elems, LANES)
        return dot(hi, one) + dot(lo, one)

    fixes = (placed(2), placed(3))

    for t in range(tiles):
        for f in range(5):
            for fix, end in zip(fixes, (0, ORDER)):
                add_face_rows(acc, f, t, 2, end, fix[f * PAD : f * PAD + FACE, tile_cols(t)])


def span_side(other_pair, staged, index, ghosts, received, acc, whole, wall, tile=None):
    slab_odd = axis_parity("span")
    for n, side in ((0, -1), (1, 1)):
        @pl.when(slab_odd == (1 - n if other_pair == 0 else n))
        def _():
            elems = index.shape[1]
            if tile in (None, 0):
                hi, lo = halves(received[...])
                one = one_hot(index[n : n + 1, :] - elems, LANES)
                whole[...] = ghosts[n] + (dot(hi, one) + dot(lo, one))
            for t in range(staged.shape[1]) if tile is None else (tile,):
                at_wall = None
                if wall is not None:
                    at_wall = jnp.logical_and(index[n : n + 1, tile_cols(t)] >= elems, wall)
                side_terms(staged, whole, acc, 1, side, t, wall=at_wall)


def late_kernel(slabs, staged, index, ghosts, sp_b, part, acc, whole):
    del part
    slab = lax.axis_index("span")
    span_side(1, staged, index, ghosts, sp_b, acc, whole, jnp.logical_or(slab == 0, slab == slabs - 1))


def last_kernel(staged, picks, th_b, part, fields_out, store_out, acc, fresh, ghost, sems):
    del part
    tiles = staged.shape[1]
    odd = axis_parity("blk")
    hi, lo = halves(th_b[...])
    ghost[...] = dot(hi, picks[...]) + dot(lo, picks[...])
    copies = []
    for t in range(tiles):
        @pl.when(odd == 0)
        def _():
            theta_side(staged, ghost, acc, -1, t)

        @pl.when(odd == 1)
        def _():
            theta_side(staged, ghost, acc, 1, t)

        for f in range(5):
            fresh[f, t, 0:VOL, :] = staged[f, t, 0:VOL, :] + section_gain * acc[f, t, 0:VOL, :]
        cols = pl.ds(t * LANES, LANES)
        pair = [
            pltpu.make_async_copy(acc.at[:, t, 0:VOL, :], store_out.at[:, :, cols], sems.at[t, 0]),
            pltpu.make_async_copy(fresh.at[:, t, 0:VOL, :], fields_out.at[:, :, cols], sems.at[t, 1]),
        ]
        for copy in pair:
            copy.start()
        copies += pair
    for copy in copies:
        copy.wait()


def params(limit=VMEM_LIMIT):
    return pltpu.CompilerParams(vmem_limit_bytes=limit)


def vmem_spec():
    return pl.BlockSpec(memory_space=pltpu.VMEM)


def hbm_spec():
    return pl.BlockSpec(memory_space=pltpu.HBM)


def in_hbm(x):
    return pltpu.with_memory_space_constraint(x, pltpu.HBM)


def in_vmem(x):
    return pltpu.with_memory_space_constraint(x, pltpu.VMEM)


def reaches(sectors):
    steps = [1 << bit for bit in range(sectors.bit_length() - 1)]
    return steps[:1] + steps[:0:-1]


def on_device(fields, section_store, mean_velocity, sound_speed, element_slot, face_turn, rotor_offset):
    per_theta, per_span = face_turn.shape
    elems = element_slot.shape[0]
    axial = elems // (per_theta * per_span)
    sectors, slabs = lax.axis_size("blk"), lax.axis_size("span")
    tiles = elems // LANES
    rows = VALS * PAD
    assert per_theta == 1 and axial == LANES and sectors % 2 == 0 and sectors & (sectors - 1) == 0
    assert 2 * per_span * VALS < LANES and FACE + tiles <= PAD
    dma = pltpu.SemaphoreType.DMA
    theta_rows = VALS * FACE + 1
    vmem, hbm = pltpu.VMEM, pltpu.HBM
    slot_h = in_hbm(element_slot.reshape(1, elems))
    stack = [vmem((8 * PAD, LANES), BF), vmem((8 * PAD, LANES), BF)]
    staged, th_a, iface, slot_v, plan, own_packed, forward_t = pl.pallas_call(
        functools.partial(first_kernel, per_span, axial, sectors),
        out_shape=(
            vmem((9, tiles, LANES, LANES), F32),
            hbm((theta_rows, elems), F32),
            vmem((PAD, LANES), F32),
            vmem((1, elems), jnp.int32),
            vmem((8, LANES), jnp.int32),
            vmem((PAD, LANES), F32),
            vmem((PAD, 8 * PAD), BF),
        ),
        in_specs=[hbm_spec()] * 9,
        out_specs=(vmem_spec(), hbm_spec()) + (vmem_spec(),) * 5,
        scratch_shapes=[
            vmem((theta_rows, elems), F32),
            vmem((PAD, 8 * PAD), BF),
            vmem((2 * rows, elems), BF),
            vmem((2 * rows, elems), BF),
            *stack,
            pltpu.SMEM((elems,), jnp.int32),
            pltpu.SMEM((per_theta, per_span), jnp.int32),
            pltpu.SMEM((per_span,), jnp.int32),
            dma((tiles, 3)),
            dma((6,)),
            dma(()),
        ],
        compiler_params=params(),
        name="first",
    )(
        in_hbm(element_slot), in_hbm(face_turn), in_hbm(rotor_offset), slot_h, in_hbm(fields), in_hbm(mean_velocity), in_hbm(sound_speed),
        in_hbm(jnp.asarray(turn_matrix(True))), in_hbm(jnp.asarray(turn_matrix(False))),
    )

    pieces, far = [iface], [0]
    near_a = lax.ppermute(th_a, "blk", [(i, i ^ 1) for i in range(sectors)])
    for reach in reaches(sectors):
        block = jnp.concatenate(pieces, 0)
        pieces.append(lax.ppermute(block, "blk", [(i, i ^ reach) for i in range(sectors)]))
        far += [k ^ reach for k in far]

    th_b, sp_a, sp_b, index, rows_hi, rows_lo = pl.pallas_call(
        functools.partial(second_kernel, per_span, axial),
        out_shape=(
            hbm((theta_rows, elems), F32),
            vmem((rows, LANES), F32),
            vmem((rows, LANES), F32),
            vmem((8, elems), jnp.int32),
            vmem((len(LOCAL_FACES) * rows, elems), BF),
            vmem((len(LOCAL_FACES) * rows, elems), BF),
        ),
        in_specs=[vmem_spec()] * 2,
        out_specs=(hbm_spec(),) + (vmem_spec(),) * 5,
        scratch_shapes=[vmem((theta_rows, elems), F32), dma(())],
        compiler_params=params(),
        name="second",
    )(in_vmem(slot_v), in_vmem(staged))
    pairs = [(i, (i + 1 if i % 2 else i - 1) % sectors) for i in range(sectors)]
    near_b = lax.ppermute(th_b, "blk", pairs)
    span_a = lax.ppermute(sp_a, "span", [(i, i ^ 1) for i in range(slabs) if i ^ 1 < slabs])
    pairs = [(i, i + 1 if i % 2 else i - 1) for i in range(slabs)]
    span_b = lax.ppermute(sp_b, "span", [(i, j) for i, j in pairs if 0 <= j < slabs])

    ghosts = pl.pallas_call(
        local_kernel,
        out_shape=vmem((len(LOCAL_FACES), rows, elems), F32),
        in_specs=[vmem_spec()] * 3,
        out_specs=vmem_spec(),
        compiler_params=params(),
        name="local",
    )(in_vmem(index), in_vmem(rows_hi), in_vmem(rows_lo))

    part = None
    block = (5, tiles, LANES, LANES)
    for place in range(2):
        work = pl.pallas_call(
            functools.partial(work_kernel if place else work_start, place, per_span),
            out_shape=vmem(block, F32),
            in_specs=[vmem_spec()] * 3 + [hbm_spec()] * 2 + [vmem_spec()] * (place > 0),
            out_specs=vmem_spec(),
            scratch_shapes=[
                vmem(block, F32),
                dma((tiles,)),
                vmem((2 * LANES, 3 * LANES), BF),
                vmem((tiles // 2, 5, 3 * LANES, 2 * LANES), BF),
                vmem((tiles // 2, 5, 3 * LANES, 2 * LANES), BF),
                dma(()),
            ],
            input_output_aliases={5: 0} if place else {},
            compiler_params=params(),
        )
        operands = [in_vmem(staged), in_vmem(index), in_vmem(ghosts)]
        operands += [in_hbm(jnp.asarray(volume_matrix())), in_hbm(section_store)]
        if place:
            operands.append(in_vmem(part))
        part = work(*operands)

    part = pl.pallas_call(
        face_kernel,
        out_shape=vmem(block, F32),
        in_specs=[vmem_spec()] * 8,
        out_specs=vmem_spec(),
        scratch_shapes=[vmem((rows, elems), F32), vmem((theta_rows, elems), F32)],
        input_output_aliases={7: 0},
        compiler_params=params(),
        name="faces",
    )(
        in_vmem(slot_v), in_vmem(staged), in_vmem(index), in_vmem(ghosts), in_vmem(near_a), in_vmem(span_a),
        in_vmem(pieces[1]), in_vmem(part),
    )

    part, picks = pl.pallas_call(
        functools.partial(interface_kernel, per_span, sectors, len(pieces), far),
        out_shape=(vmem(block, F32), vmem((elems, elems), BF)),
        in_specs=[vmem_spec()] * (6 + len(pieces)),
        out_specs=(vmem_spec(),) * 2,
        scratch_shapes=stack,
        input_output_aliases={5: 0},
        compiler_params=params(),
        name="interface",
    )(
        in_vmem(plan), in_vmem(slot_v), in_vmem(index), in_vmem(own_packed), in_vmem(forward_t), in_vmem(part),
        *[in_vmem(piece) for piece in pieces],
    )

    part = pl.pallas_call(
        functools.partial(late_kernel, slabs),
        out_shape=vmem(block, F32),
        in_specs=[vmem_spec()] * 5,
        out_specs=vmem_spec(),
        scratch_shapes=[vmem((rows, elems), F32)],
        input_output_aliases={4: 0},
        compiler_params=params(),
        name="late",
    )(in_vmem(staged), in_vmem(index), in_vmem(ghosts), in_vmem(span_b), in_vmem(part))

    whole = hbm((5, VOL, elems), F32)
    fields_next, store_next, _ = pl.pallas_call(
        last_kernel,
        out_shape=(whole, whole, vmem(block, F32)),
        in_specs=[vmem_spec()] * 4,
        out_specs=(hbm_spec(),) * 2 + (vmem_spec(),),
        scratch_shapes=[vmem(block, F32), vmem((theta_rows, elems), F32), dma((tiles, 2))],
        input_output_aliases={3: 2},
        compiler_params=params(),
        name="last",
    )(in_vmem(staged), in_vmem(picks), in_vmem(near_b), in_vmem(part))
    return fields_next, store_next


def solution(mesh):
    both = ("blk", "span")
    in_specs = (
        P(None, None, both),
        P(None, None, both),
        P(None, None, both),
        P(None, both),
        P(both),
        P("blk", "span"),
        P("span"),
    )
    out_specs = (P(None, None, both), P(None, None, both))
    return jax.shard_map(on_device, mesh=mesh, in_specs=in_specs, out_specs=out_specs, check_vma=False)
```

```python
import functools

import jax
import jax.numpy as jnp
import numpy as np
from jax import lax
from jax.experimental import pallas as pl
from jax.experimental.pallas import tpu as pltpu
from jax.sharding import PartitionSpec as P


ORDER = 4
NODE = ORDER + 1
FACE = NODE * NODE
VOL = NODE**3
LANES = 128
PAD = 32
VALS = 7

section_decay = -567301805773.0 / 1357537059087.0
section_gain = 5161836677717.0 / 13612068292357.0
time_step = 0.05
metric_scale = (1.0, 1.5, 0.75)
end_weight = 0.1

BF = jnp.bfloat16
F32 = jnp.float32
VMEM_LIMIT = 24 * 1024 * 1024


def lobatto_slopes():
    inner_root = np.sqrt(3.0 / 7.0)
    points = np.array([-1.0, -inner_root, 0.0, inner_root, 1.0])
    count = points.shape[0]
    slopes = np.zeros((count, count))
    for r in range(count):
        for c in range(count):
            if r == c:
                slopes[r, c] = sum(1.0 / (points[r] - points[o]) for o in range(count) if o != r)
            else:
                top = np.prod([points[r] - points[o] for o in range(count) if o != r])
                low = np.prod([points[c] - points[o] for o in range(count) if o != c])
                slopes[r, c] = top / (low * (points[r] - points[c]))
    return slopes


def split_np(table):
    high = np.asarray(table, np.float32).astype(BF)
    low = (np.asarray(table, np.float64) - high.astype(np.float64)).astype(BF)
    return high, low


def volume_matrix():
    slopes = lobatto_slopes()
    eye = np.eye(NODE)
    parts = (
        np.kron(np.kron(slopes, eye), eye),
        np.kron(np.kron(eye, slopes), eye),
        np.kron(np.kron(eye, eye), slopes),
    )
    full = np.zeros((LANES, 3 * LANES))
    for d in range(3):
        full[:VOL, d * LANES : d * LANES + VOL] = -time_step * metric_scale[d] * parts[d]
    high, low = split_np(full)
    return np.concatenate([high, low], 0)


def turn_matrix(inverse):
    table = np.zeros((PAD, 8 * PAD), np.float32)
    for code in range(8):
        index = np.arange(FACE).reshape(NODE, NODE)
        if inverse:
            if code & 2:
                index = index[:, ::-1]
            if code & 1:
                index = index[::-1, :]
            if code & 4:
                index = index.T
        else:
            if code & 4:
                index = index.T
            if code & 1:
                index = index[::-1, :]
            if code & 2:
                index = index[:, ::-1]
        for n, o in enumerate(index.reshape(-1)):
            table[n, code * PAD + o] = 1.0
    return table.astype(BF)


def dot(a, b):
    return jnp.dot(a, b, preferred_element_type=F32)


def dot_t(a, b):
    return lax.dot_general(a, b, (((1,), (1,)), ((), ())), preferred_element_type=F32)


def halves(x):
    high = x.astype(BF)
    return high, (x - high.astype(F32)).astype(BF)


def lane_iota(shape):
    return lax.broadcasted_iota(jnp.int32, shape, len(shape) - 1)


def face_rows(ref, v, tile, d, end):
    if d == 0:
        return ref[v, tile, pl.ds(end * FACE, FACE), :]
    if d == 1:
        starts = [i * FACE + end * NODE for i in range(NODE)]
        return jnp.concatenate([ref[v, tile, pl.ds(s, NODE), :] for s in starts], axis=0)
    return ref[v, tile, pl.ds(end, FACE, NODE), :]


def add_face_rows(ref, v, tile, d, end, value):
    if d == 0:
        ref[v, tile, pl.ds(end * FACE, FACE), :] += value
    elif d == 1:
        for i in range(NODE):
            ref[v, tile, pl.ds(i * FACE + end * NODE, NODE), :] += value[i * NODE : (i + 1) * NODE]
    else:
        ref[v, tile, pl.ds(end, FACE, NODE), :] += value


def value_index(f, d):
    return f if f < 5 else (5 + d if f == 5 else 8)


def surface(own, other, d, side):
    qo, mo, co = own[:5], own[5], own[6]
    qn, mn, cn = other[:5], other[5], other[6]
    reach = jnp.maximum(jnp.abs(mo) + co, jnp.abs(mn) + cn)
    weight = side * 0.5 * time_step * metric_scale[d] / end_weight
    if side > 0:
        ao, an = mo - reach, mn - reach
    else:
        ao, an = mo + reach, mn + reach
    velocity_part = co * qo[1 + d] - cn * qn[1 + d]
    pressure_part = co * qo[4] - cn * qn[4]
    out = []
    for f in range(5):
        x = ao * qo[f] - an * qn[f]
        if f in (0, 4):
            x = x + velocity_part
        elif f == 1 + d:
            x = x + pressure_part
        out.append(weight * x)
    return out


def axis_parity(axis):
    return lax.rem(lax.axis_index(axis), 2)


def one_hot(index_row, count):
    short = jnp.broadcast_to(index_row, (16, index_row.shape[1])).astype(jnp.int16)
    rows = lax.broadcasted_iota(jnp.int16, (16, index_row.shape[1]), 0)
    one, zero = jnp.ones(short.shape, BF), jnp.zeros(short.shape, BF)
    return jnp.concatenate([jnp.where(rows == short - r, one, zero) for r in range(0, count, 16)], 0)


def store_halves(ref_hi, ref_lo, at, cols, value):
    hi, lo = halves(jnp.concatenate([value, jnp.zeros((PAD - FACE, value.shape[1]), F32)], 0))
    ref_hi[at : at + PAD, cols] = hi
    ref_lo[at : at + PAD, cols] = lo


def turned(packed, code, turn_t, stack_hi, stack_lo):
    hi = packed.astype(BF).astype(F32)
    lo = packed - hi
    for c in range(8):
        stack_hi[c * PAD : (c + 1) * PAD, :] = jnp.where(code == c, hi, 0.0).astype(BF)
        stack_lo[c * PAD : (c + 1) * PAD, :] = jnp.where(code == c, lo, 0.0).astype(BF)
    return dot(turn_t[...], stack_hi[...]) + dot(turn_t[...], stack_lo[...])


def tile_cols(t):
    return slice(t * LANES, (t + 1) * LANES)


def neighbour_index(rows, slot_v):
    elems = slot_v.shape[1]
    own = one_hot(slot_v[...], elems)
    base = 256.0
    table = jnp.concatenate(rows + [jnp.zeros((8 - len(rows), elems), F32)], 0)
    upper = jnp.floor(table * (1.0 / base))
    lower = table - upper * base
    both = jnp.concatenate([upper, lower], 0).astype(BF)
    moved = dot_t(both, own)
    return (moved[0:8] * base + moved[8:16]).astype(jnp.int32)


def first_kernel(
    per_span, axial, sectors, slot_l, turn_l, offset_l, slot_h, fields, velocity, sound, turn_h, forward_h,
    staged, theta, iface, slot_v, plan, own_packed, forward_t, turn_t, rows_hi, rows_lo, stack_hi, stack_lo, slot_s, turn_s, offset_s,
    sems, small_sems,
):
    elems = slot_v.shape[1]
    tiles = elems // LANES
    half = axial // 2
    rows = VALS * PAD
    small = [
        pltpu.make_async_copy(slot_h, slot_v, small_sems.at[0]),
        pltpu.make_async_copy(turn_h, turn_t, small_sems.at[1]),
        pltpu.make_async_copy(slot_l, slot_s, small_sems.at[2]),
        pltpu.make_async_copy(turn_l, turn_s, small_sems.at[3]),
        pltpu.make_async_copy(offset_l, offset_s, small_sems.at[4]),
        pltpu.make_async_copy(forward_h, forward_t, small_sems.at[5]),
    ]
    loads = []
    for t in range(tiles):
        cols = pl.ds(t * LANES, LANES)
        loads.append([
            pltpu.make_async_copy(fields.at[:, :, cols], staged.at[0:5, t, 0:VOL, :], sems.at[t, 0]),
            pltpu.make_async_copy(velocity.at[:, :, cols], staged.at[5:8, t, 0:VOL, :], sems.at[t, 1]),
            pltpu.make_async_copy(sound.at[:, cols], staged.at[8, t, 0:VOL, :], sems.at[t, 2]),
        ])
        for copy in loads[-1]:
            copy.start()
    for copy in small:
        copy.start()
    for copy in small:
        copy.wait()
    sector = lax.axis_index("blk")
    lane = lane_iota((1, LANES))
    column = lane % (2 * per_span)
    target = jnp.full((1, LANES), -1, jnp.int32)
    code = jnp.zeros((1, LANES), jnp.int32)
    want = jnp.zeros((1, LANES), jnp.int32)
    forward = jnp.zeros((1, LANES), jnp.int32)
    for s in range(per_span):
        target = jnp.where(lane == s, slot_s[s * axial + half - 1], target)
        target = jnp.where(lane == per_span + s, slot_s[s * axial + half], target)
        code = jnp.where(column == per_span + s, turn_s[0, s], code)
        forward = jnp.where(column == s, turn_s[0, s], forward)
        shift = lax.rem(offset_s[s], sectors)
        want = jnp.where(column == s, lax.rem(sector - shift + sectors, sectors), want)
        want = jnp.where(column == per_span + s, lax.rem(sector + shift, sectors), want)
    plan[0:1, :] = want
    plan[1:2, :] = forward
    one = one_hot(target, elems)
    theta[VALS * FACE : VALS * FACE + 1, :] = jnp.zeros((1, elems), F32)
    odd = axis_parity("blk")

    for t in range(tiles):
        for copy in loads[t]:
            copy.wait()
        cols = tile_cols(t)

        @pl.when(odd == 0)
        def _():
            for f in range(VALS):
                theta[f * FACE : (f + 1) * FACE, cols] = face_rows(staged, value_index(f, 0), t, 0, ORDER)

        @pl.when(odd == 1)
        def _():
            for f in range(VALS):
                theta[f * FACE : (f + 1) * FACE, cols] = face_rows(staged, value_index(f, 0), t, 0, 0)

        for n, end in enumerate((ORDER, 0)):
            for f in range(VALS):
                at = n * rows + f * PAD
                store_halves(rows_hi, rows_lo, at, cols, face_rows(staged, value_index(f, 2), t, 2, end))
    both = dot(rows_hi[...], one) + dot(rows_lo[...], one)
    both = jnp.where(lane < per_span, both[0:rows], jnp.where(lane < 2 * per_span, both[rows:], 0.0))
    packed = both[0:PAD]
    for f in range(1, VALS):
        packed = packed + pltpu.roll(both[f * PAD : (f + 1) * PAD], f * 2 * per_span, 1)
    own_packed[...] = packed
    iface[...] = turned(packed, code, turn_t, stack_hi, stack_lo)
    for t in range(tiles):
        iface[PAD - tiles + t : PAD - tiles + t + 1, :] = slot_v[:, tile_cols(t)].astype(F32)


LOCAL_FACES = ((1, 1), (1, 0), (2, 1), (2, 0))


def second_kernel(
    per_span, axial, slot_v, staged, matrix_h, theta, sp_a, sp_b, index, rows_hi, rows_lo, matrix, sem,
):
    load = pltpu.make_async_copy(matrix_h, matrix, sem)
    load.start()
    elems = slot_v.shape[1]
    tiles = elems // LANES
    half = axial // 2
    rows = VALS * PAD
    theta[VALS * FACE : VALS * FACE + 1, :] = jnp.zeros((1, elems), F32)
    odd = axis_parity("blk")

    @pl.when(odd == 0)
    def _():
        for t in range(tiles):
            for f in range(VALS):
                theta[f * FACE : (f + 1) * FACE, tile_cols(t)] = face_rows(staged, value_index(f, 0), t, 0, 0)

    @pl.when(odd == 1)
    def _():
        for t in range(tiles):
            for f in range(VALS):
                theta[f * FACE : (f + 1) * FACE, tile_cols(t)] = face_rows(staged, value_index(f, 0), t, 0, ORDER)

    for n, (d, end) in enumerate(LOCAL_FACES):
        for t in range(tiles):
            for f in range(VALS):
                x = face_rows(staged, value_index(f, d), t, d, end * ORDER)
                store_halves(rows_hi, rows_lo, n * rows + f * PAD, tile_cols(t), x)

    def gathered(start, row):
        one = one_hot(row, elems)
        return dot(rows_hi[start : start + rows, :], one) + dot(rows_lo[start : start + rows, :], one)

    high = gathered(0, slot_v[:, elems - axial : elems])
    low = gathered(rows, slot_v[:, 0:axial])
    span_odd = axis_parity("span")

    @pl.when(span_odd == 0)
    def _():
        sp_a[...] = high
        sp_b[...] = low

    @pl.when(span_odd == 1)
    def _():
        sp_a[...] = low
        sp_b[...] = high

    slots = slot_v[...].astype(F32)
    lane = lane_iota((1, elems))
    position = lane % axial
    row = (lane // axial).astype(F32)
    lanes_f = lane.astype(F32)
    span_low = jnp.where(lane < axial, elems + lanes_f, pltpu.roll(slots, axial, 1))
    span_high = jnp.where(lane >= elems - axial, axial + lanes_f, pltpu.roll(slots, elems - axial, 1))
    none = elems + LANES - 1.0
    ax_low = jnp.where(position == half, elems + row, pltpu.roll(slots, 1, 1))
    ax_low = jnp.where(position == 0, none, ax_low)
    ax_high = jnp.where(position == half - 1, elems + per_span + row, pltpu.roll(slots, elems - 1, 1))
    ax_high = jnp.where(position == axial - 1, none, ax_high)
    index[...] = neighbour_index([span_low, span_high, ax_low, ax_high], slot_v)
    load.wait()


def local_kernel(index, rows_hi, rows_lo, ghosts):
    elems = index.shape[1]
    rows = VALS * PAD
    for n in range(len(LOCAL_FACES)):
        one = one_hot(index[n : n + 1, :], elems)
        at = slice(n * rows, (n + 1) * rows)
        ghosts[n] = dot(rows_hi[at, :], one) + dot(rows_lo[at, :], one)


def work_kernel(place, per_span, staged, index, ghosts, matrix, store_h, earlier, out, store, sems, *scratch):
    del earlier

    @pl.when(work_place() == place)
    def _():
        tiles = staged.shape[1]
        elems = tiles * LANES
        stores = [
            pltpu.make_async_copy(store_h.at[:, :, pl.ds(t * LANES, LANES)], store.at[:, t, 0:VOL, :], sems.at[t])
            for t in range(tiles)
        ]
        for copy in stores:
            copy.start()
        volume_terms(staged, matrix, out, *scratch)
        for copy in stores:
            copy.wait()
        for t in range(tiles):
            for f in range(5):
                out[f, t, 0:VOL, :] += section_decay * store[f, t, 0:VOL, :]
            for n, side in ((2, -1), (3, 1)):
                at = index[n : n + 1, tile_cols(t)]
                keep = jnp.logical_or(at < elems, at >= elems + 2 * per_span)
                side_terms(staged, ghosts.at[n], out, 2, side, t, keep=keep)


def work_start(place, per_span, staged, index, ghosts, matrix, store_h, out, *scratch):
    work_kernel(place, per_span, staged, index, ghosts, matrix, store_h, None, out, *scratch)


def work_place():
    return jnp.where(axis_parity("span") == 1, 0, 1)


def volume_terms(staged, matrix, out, flux_hi, flux_lo):
    tiles = staged.shape[1]
    step = 16
    for pair in range(tiles // 2):
        for half in range(2):
            t = 2 * pair + half
            cols = tile_cols(half)
            for r in range(0, VOL, step):
                n = min(step, VOL - r)
                rows = slice(r, r + n)
                q = [staged[f, t, rows, :] for f in range(5)]
                c = staged[8, t, rows, :]
                cp = c * q[4]
                for d in range(3):
                    m = staged[5 + d, t, rows, :]
                    cu = c * q[1 + d]
                    for f in range(5):
                        x = m * q[f]
                        if f in (0, 4):
                            x = x + cu
                        elif f == 1 + d:
                            x = x + cp
                        if n < step:
                            x = jnp.concatenate([x, jnp.zeros((step - n, LANES), F32)], 0)
                        hi, lo = halves(x)
                        flux_hi[pair, f, d * LANES + r : d * LANES + r + step, cols] = hi
                        flux_lo[pair, f, d * LANES + r : d * LANES + r + step, cols] = lo
        for f in range(5):
            a = dot(matrix[...], flux_hi[pair, f])
            b = dot(matrix[0:LANES, :], flux_lo[pair, f])
            total = a[0:LANES] + a[LANES : 2 * LANES] + b
            for half in range(2):
                out[f, 2 * pair + half] = total[:, tile_cols(half)]


def theta_ghost(recv, index_row):
    one = one_hot(index_row, recv.shape[1])
    hi, lo = halves(recv[...])
    return dot(hi, one) + dot(lo, one)


def theta_side(staged, ghost, acc, side, t):
    start = ORDER * FACE if side > 0 else 0
    own = [staged[value_index(f, 0), t, start : start + FACE, :] for f in range(VALS)]
    other = [ghost[f * FACE : (f + 1) * FACE, tile_cols(t)] for f in range(VALS)]
    for f, x in enumerate(surface(own, other, 0, side)):
        acc[f, t, start : start + FACE, :] += x


def side_terms(staged, ghost_ref, acc, d, side, t, keep=None, wall=None):
    cols = tile_cols(t)
    end = ORDER if side > 0 else 0
    own = [face_rows(staged, value_index(f, d), t, d, end) for f in range(VALS)]
    other = [ghost_ref[f * PAD : f * PAD + FACE, cols] for f in range(VALS)]
    if wall is not None:
        for f in range(VALS):
            other[f] = jnp.where(wall, -own[f] if f == 1 + d else own[f], other[f])
    for f, x in enumerate(surface(own, other, d, side)):
        add_face_rows(acc, f, t, d, end, x if keep is None else jnp.where(keep, x, 0.0))


def face_kernel(slot_v, staged, index, ghosts, th_a, sp_a, iface_a, part, acc, whole, ghost):
    del part
    tiles = staged.shape[1]
    odd = axis_parity("blk")
    slots_a = jnp.concatenate([iface_a[PAD - tiles + t : PAD - tiles + t + 1, :] for t in range(tiles)], 1)
    ghost[...] = theta_ghost(th_a, neighbour_index([slots_a], slot_v)[0:1])
    span_side(0, staged, index, ghosts, sp_a, acc, whole, None)
    for t in range(tiles):
        @pl.when(odd == 0)
        def _():
            theta_side(staged, ghost, acc, 1, t)

        @pl.when(odd == 1)
        def _():
            theta_side(staged, ghost, acc, -1, t)


def interface_kernel(
    per_span, sectors, pieces, far,
    plan, slot_v, index, own_packed, turn_t, part, *rest,
):
    del part
    iface = rest[:pieces]
    acc, picks, stack_hi, stack_lo = rest[pieces:]
    elems = slot_v.shape[1]
    tiles = elems // LANES
    sector = lax.axis_index("blk")
    odd = lax.rem(sector, 2)

    partner = lax.rem(sector + jnp.where(odd == 1, 1, sectors - 1), sectors)
    slots_b = jnp.zeros((tiles, LANES), F32)
    want, code = plan[0:1, :], plan[1:2, :]
    near = jnp.zeros((PAD, LANES), F32)
    blocks = [piece[b * PAD : (b + 1) * PAD, :] for piece in iface for b in range(piece.shape[0] // PAD)]
    for k, block in zip(far, blocks):
        near = jnp.where(want == (sector ^ k), block, near)
        slots_b = jnp.where(partner == (sector ^ k), block[PAD - tiles :], slots_b)
    flat = lambda x: jnp.concatenate([x[t : t + 1] for t in range(tiles)], 1)
    picks[...] = one_hot(neighbour_index([flat(slots_b)], slot_v)[0:1], elems)

    near = turned(near, code, turn_t, stack_hi, stack_lo)
    lane = lane_iota((1, LANES))
    used = lane < 2 * per_span
    own, other = [], []
    for f in range(VALS):
        at = f * 2 * per_span
        down = pltpu.roll(own_packed[...], LANES - at - per_span, 1)
        up = pltpu.roll(own_packed[...], (LANES - at + per_span) % LANES, 1)
        own.append(jnp.where(used, jnp.where(lane < per_span, down, up), 0.0))
        theirs = near if f == 0 else pltpu.roll(near, LANES - at, 1)
        other.append(jnp.where(used, theirs, 0.0))
    low = surface(own, other, 2, -1)
    high = surface(own, other, 2, 1)
    terms = jnp.concatenate([jnp.where(lane < per_span, x, y) for x, y in zip(low, high)], 0)
    hi, lo = halves(jnp.where(used, terms, 0.0))

    def placed(n):
        one = one_hot(index[n : n + 1, :] - elems, LANES)
        return dot(hi, one) + dot(lo, one)

    fixes = (placed(2), placed(3))

    for t in range(tiles):
        for f in range(5):
            for fix, end in zip(fixes, (0, ORDER)):
                add_face_rows(acc, f, t, 2, end, fix[f * PAD : f * PAD + FACE, tile_cols(t)])


def span_side(other_pair, staged, index, ghosts, received, acc, whole, wall, tile=None):
    slab_odd = axis_parity("span")
    for n, side in ((0, -1), (1, 1)):
        @pl.when(slab_odd == (1 - n if other_pair == 0 else n))
        def _():
            elems = index.shape[1]
            if tile in (None, 0):
                hi, lo = halves(received[...])
                one = one_hot(index[n : n + 1, :] - elems, LANES)
                whole[...] = ghosts[n] + (dot(hi, one) + dot(lo, one))
            for t in range(staged.shape[1]) if tile is None else (tile,):
                at_wall = None
                if wall is not None:
                    at_wall = jnp.logical_and(index[n : n + 1, tile_cols(t)] >= elems, wall)
                side_terms(staged, whole, acc, 1, side, t, wall=at_wall)


def late_kernel(slabs, staged, index, ghosts, sp_b, part, acc, whole):
    del part
    slab = lax.axis_index("span")
    span_side(1, staged, index, ghosts, sp_b, acc, whole, jnp.logical_or(slab == 0, slab == slabs - 1))


def last_kernel(staged, picks, th_b, part, fields_out, store_out, acc, fresh, ghost, sems):
    del part
    tiles = staged.shape[1]
    odd = axis_parity("blk")
    hi, lo = halves(th_b[...])
    ghost[...] = dot(hi, picks[...]) + dot(lo, picks[...])
    copies = []
    for t in range(tiles):
        @pl.when(odd == 0)
        def _():
            theta_side(staged, ghost, acc, -1, t)

        @pl.when(odd == 1)
        def _():
            theta_side(staged, ghost, acc, 1, t)

        for f in range(5):
            fresh[f, t, 0:VOL, :] = staged[f, t, 0:VOL, :] + section_gain * acc[f, t, 0:VOL, :]
        cols = pl.ds(t * LANES, LANES)
        pair = [
            pltpu.make_async_copy(acc.at[:, t, 0:VOL, :], store_out.at[:, :, cols], sems.at[t, 0]),
            pltpu.make_async_copy(fresh.at[:, t, 0:VOL, :], fields_out.at[:, :, cols], sems.at[t, 1]),
        ]
        for copy in pair:
            copy.start()
        copies += pair
    for copy in copies:
        copy.wait()


def params(limit=VMEM_LIMIT):
    return pltpu.CompilerParams(vmem_limit_bytes=limit)


def vmem_spec():
    return pl.BlockSpec(memory_space=pltpu.VMEM)


def hbm_spec():
    return pl.BlockSpec(memory_space=pltpu.HBM)


def in_hbm(x):
    return pltpu.with_memory_space_constraint(x, pltpu.HBM)


def in_vmem(x):
    return pltpu.with_memory_space_constraint(x, pltpu.VMEM)


def reaches(sectors):
    steps = [1 << bit for bit in range(sectors.bit_length() - 1)]
    return steps[:1] + steps[:0:-1]


def on_device(fields, section_store, mean_velocity, sound_speed, element_slot, face_turn, rotor_offset):
    per_theta, per_span = face_turn.shape
    elems = element_slot.shape[0]
    axial = elems // (per_theta * per_span)
    sectors, slabs = lax.axis_size("blk"), lax.axis_size("span")
    tiles = elems // LANES
    rows = VALS * PAD
    assert per_theta == 1 and axial == LANES and sectors % 2 == 0 and sectors & (sectors - 1) == 0
    assert 2 * per_span * VALS < LANES and FACE + tiles <= PAD
    dma = pltpu.SemaphoreType.DMA
    theta_rows = VALS * FACE + 1
    vmem, hbm = pltpu.VMEM, pltpu.HBM
    slot_h = in_hbm(element_slot.reshape(1, elems))
    stack = [vmem((8 * PAD, LANES), BF), vmem((8 * PAD, LANES), BF)]
    staged, th_a, iface, slot_v, plan, own_packed, forward_t = pl.pallas_call(
        functools.partial(first_kernel, per_span, axial, sectors),
        out_shape=(
            vmem((9, tiles, LANES, LANES), F32),
            vmem((theta_rows, elems), F32),
            vmem((PAD, LANES), F32),
            vmem((1, elems), jnp.int32),
            vmem((8, LANES), jnp.int32),
            vmem((PAD, LANES), F32),
            vmem((PAD, 8 * PAD), BF),
        ),
        in_specs=[hbm_spec()] * 9,
        out_specs=(vmem_spec(),) * 7,
        scratch_shapes=[
            vmem((PAD, 8 * PAD), BF),
            vmem((2 * rows, elems), BF),
            vmem((2 * rows, elems), BF),
            *stack,
            pltpu.SMEM((elems,), jnp.int32),
            pltpu.SMEM((per_theta, per_span), jnp.int32),
            pltpu.SMEM((per_span,), jnp.int32),
            dma((tiles, 3)),
            dma((6,)),
        ],
        compiler_params=params(),
        name="first",
    )(
        in_hbm(element_slot), in_hbm(face_turn), in_hbm(rotor_offset), slot_h, in_hbm(fields), in_hbm(mean_velocity), in_hbm(sound_speed),
        in_hbm(jnp.asarray(turn_matrix(True))), in_hbm(jnp.asarray(turn_matrix(False))),
    )

    pieces, far = [iface], [0]
    near_a = lax.ppermute(th_a, "blk", [(i, i ^ 1) for i in range(sectors)])
    for reach in reaches(sectors):
        block = jnp.concatenate(pieces, 0)
        pieces.append(lax.ppermute(block, "blk", [(i, i ^ reach) for i in range(sectors)]))
        far += [k ^ reach for k in far]

    th_b, sp_a, sp_b, index, rows_hi, rows_lo, matrix = pl.pallas_call(
        functools.partial(second_kernel, per_span, axial),
        out_shape=(
            vmem((theta_rows, elems), F32),
            vmem((rows, LANES), F32),
            vmem((rows, LANES), F32),
            vmem((8, elems), jnp.int32),
            vmem((len(LOCAL_FACES) * rows, elems), BF),
            vmem((len(LOCAL_FACES) * rows, elems), BF),
            vmem((2 * LANES, 3 * LANES), BF),
        ),
        in_specs=[vmem_spec()] * 2 + [hbm_spec()],
        out_specs=(vmem_spec(),) * 7,
        scratch_shapes=[dma(())],
        compiler_params=params(),
        name="second",
    )(in_vmem(slot_v), in_vmem(staged), in_hbm(jnp.asarray(volume_matrix())))
    pairs = [(i, (i + 1 if i % 2 else i - 1) % sectors) for i in range(sectors)]
    near_b = lax.ppermute(th_b, "blk", pairs)
    span_a = lax.ppermute(sp_a, "span", [(i, i ^ 1) for i in range(slabs) if i ^ 1 < slabs])
    pairs = [(i, i + 1 if i % 2 else i - 1) for i in range(slabs)]
    span_b = lax.ppermute(sp_b, "span", [(i, j) for i, j in pairs if 0 <= j < slabs])

    ghosts = pl.pallas_call(
        local_kernel,
        out_shape=vmem((len(LOCAL_FACES), rows, elems), F32),
        in_specs=[vmem_spec()] * 3,
        out_specs=vmem_spec(),
        compiler_params=params(),
        name="local",
    )(in_vmem(index), in_vmem(rows_hi), in_vmem(rows_lo))

    part = None
    block = (5, tiles, LANES, LANES)
    for place in range(2):
        work = pl.pallas_call(
            functools.partial(work_kernel if place else work_start, place, per_span),
            out_shape=vmem(block, F32),
            in_specs=[vmem_spec()] * 4 + [hbm_spec()] + [vmem_spec()] * (place > 0),
            out_specs=vmem_spec(),
            scratch_shapes=[
                vmem(block, F32),
                dma((tiles,)),
                vmem((tiles // 2, 5, 3 * LANES, 2 * LANES), BF),
                vmem((tiles // 2, 5, 3 * LANES, 2 * LANES), BF),
            ],
            input_output_aliases={5: 0} if place else {},
            compiler_params=params(),
        )
        operands = [in_vmem(staged), in_vmem(index), in_vmem(ghosts)]
        operands += [in_vmem(matrix), in_hbm(section_store)]
        if place:
            operands.append(in_vmem(part))
        part = work(*operands)

    part = pl.pallas_call(
        face_kernel,
        out_shape=vmem(block, F32),
        in_specs=[vmem_spec()] * 8,
        out_specs=vmem_spec(),
        scratch_shapes=[vmem((rows, elems), F32), vmem((theta_rows, elems), F32)],
        input_output_aliases={7: 0},
        compiler_params=params(),
        name="faces",
    )(
        in_vmem(slot_v), in_vmem(staged), in_vmem(index), in_vmem(ghosts), in_vmem(near_a), in_vmem(span_a),
        in_vmem(pieces[1]), in_vmem(part),
    )

    part, picks = pl.pallas_call(
        functools.partial(interface_kernel, per_span, sectors, len(pieces), far),
        out_shape=(vmem(block, F32), vmem((elems, elems), BF)),
        in_specs=[vmem_spec()] * (6 + len(pieces)),
        out_specs=(vmem_spec(),) * 2,
        scratch_shapes=stack,
        input_output_aliases={5: 0},
        compiler_params=params(),
        name="interface",
    )(
        in_vmem(plan), in_vmem(slot_v), in_vmem(index), in_vmem(own_packed), in_vmem(forward_t), in_vmem(part),
        *[in_vmem(piece) for piece in pieces],
    )

    part = pl.pallas_call(
        functools.partial(late_kernel, slabs),
        out_shape=vmem(block, F32),
        in_specs=[vmem_spec()] * 5,
        out_specs=vmem_spec(),
        scratch_shapes=[vmem((rows, elems), F32)],
        input_output_aliases={4: 0},
        compiler_params=params(),
        name="late",
    )(in_vmem(staged), in_vmem(index), in_vmem(ghosts), in_vmem(span_b), in_vmem(part))

    whole = hbm((5, VOL, elems), F32)
    fields_next, store_next, _ = pl.pallas_call(
        last_kernel,
        out_shape=(whole, whole, vmem(block, F32)),
        in_specs=[vmem_spec()] * 4,
        out_specs=(hbm_spec(),) * 2 + (vmem_spec(),),
        scratch_shapes=[vmem(block, F32), vmem((theta_rows, elems), F32), dma((tiles, 2))],
        input_output_aliases={3: 2},
        compiler_params=params(),
        name="last",
    )(in_vmem(staged), in_vmem(picks), in_vmem(near_b), in_vmem(part))
    return fields_next, store_next


def solution(mesh):
    both = ("blk", "span")
    in_specs = (
        P(None, None, both),
        P(None, None, both),
        P(None, None, both),
        P(None, both),
        P(both),
        P("blk", "span"),
        P("span"),
    )
    out_specs = (P(None, None, both), P(None, None, both))
    return jax.shard_map(on_device, mesh=mesh, in_specs=in_specs, out_specs=out_specs, check_vma=False)
```

```python
import functools

import jax
import jax.numpy as jnp
import numpy as np
from jax import lax
from jax.experimental import pallas as pl
from jax.experimental.pallas import tpu as pltpu
from jax.sharding import PartitionSpec as P


ORDER = 4
NODE = ORDER + 1
FACE = NODE * NODE
VOL = NODE**3
LANES = 128
PAD = 32
VALS = 7

section_decay = -567301805773.0 / 1357537059087.0
section_gain = 5161836677717.0 / 13612068292357.0
time_step = 0.05
metric_scale = (1.0, 1.5, 0.75)
end_weight = 0.1

BF = jnp.bfloat16
F32 = jnp.float32
VMEM_LIMIT = 24 * 1024 * 1024


def lobatto_slopes():
    inner_root = np.sqrt(3.0 / 7.0)
    points = np.array([-1.0, -inner_root, 0.0, inner_root, 1.0])
    count = points.shape[0]
    slopes = np.zeros((count, count))
    for r in range(count):
        for c in range(count):
            if r == c:
                slopes[r, c] = sum(1.0 / (points[r] - points[o]) for o in range(count) if o != r)
            else:
                top = np.prod([points[r] - points[o] for o in range(count) if o != r])
                low = np.prod([points[c] - points[o] for o in range(count) if o != c])
                slopes[r, c] = top / (low * (points[r] - points[c]))
    return slopes


def split_np(table):
    high = np.asarray(table, np.float32).astype(BF)
    low = (np.asarray(table, np.float64) - high.astype(np.float64)).astype(BF)
    return high, low


def volume_matrix():
    slopes = lobatto_slopes()
    eye = np.eye(NODE)
    parts = (
        np.kron(np.kron(slopes, eye), eye),
        np.kron(np.kron(eye, slopes), eye),
        np.kron(np.kron(eye, eye), slopes),
    )
    full = np.zeros((LANES, 3 * LANES))
    for d in range(3):
        full[:VOL, d * LANES : d * LANES + VOL] = -time_step * metric_scale[d] * parts[d]
    high, low = split_np(full)
    return np.concatenate([high, low], 0)


def turn_matrix(inverse):
    table = np.zeros((PAD, 8 * PAD), np.float32)
    for code in range(8):
        index = np.arange(FACE).reshape(NODE, NODE)
        if inverse:
            if code & 2:
                index = index[:, ::-1]
            if code & 1:
                index = index[::-1, :]
            if code & 4:
                index = index.T
        else:
            if code & 4:
                index = index.T
            if code & 1:
                index = index[::-1, :]
            if code & 2:
                index = index[:, ::-1]
        for n, o in enumerate(index.reshape(-1)):
            table[n, code * PAD + o] = 1.0
    return table.astype(BF)


def dot(a, b):
    return jnp.dot(a, b, preferred_element_type=F32)


def dot_t(a, b):
    return lax.dot_general(a, b, (((1,), (1,)), ((), ())), preferred_element_type=F32)


def halves(x):
    high = x.astype(BF)
    return high, (x - high.astype(F32)).astype(BF)


def lane_iota(shape):
    return lax.broadcasted_iota(jnp.int32, shape, len(shape) - 1)


def face_rows(ref, v, tile, d, end):
    if d == 0:
        return ref[v, tile, pl.ds(end * FACE, FACE), :]
    if d == 1:
        starts = [i * FACE + end * NODE for i in range(NODE)]
        return jnp.concatenate([ref[v, tile, pl.ds(s, NODE), :] for s in starts], axis=0)
    return ref[v, tile, pl.ds(end, FACE, NODE), :]


def add_face_rows(ref, v, tile, d, end, value):
    if d == 0:
        ref[v, tile, pl.ds(end * FACE, FACE), :] += value
    elif d == 1:
        for i in range(NODE):
            ref[v, tile, pl.ds(i * FACE + end * NODE, NODE), :] += value[i * NODE : (i + 1) * NODE]
    else:
        ref[v, tile, pl.ds(end, FACE, NODE), :] += value


def value_index(f, d):
    return f if f < 5 else (5 + d if f == 5 else 8)


def surface(own, other, d, side):
    qo, mo, co = own[:5], own[5], own[6]
    qn, mn, cn = other[:5], other[5], other[6]
    reach = jnp.maximum(jnp.abs(mo) + co, jnp.abs(mn) + cn)
    weight = side * 0.5 * time_step * metric_scale[d] / end_weight
    if side > 0:
        ao, an = mo - reach, mn - reach
    else:
        ao, an = mo + reach, mn + reach
    velocity_part = co * qo[1 + d] - cn * qn[1 + d]
    pressure_part = co * qo[4] - cn * qn[4]
    out = []
    for f in range(5):
        x = ao * qo[f] - an * qn[f]
        if f in (0, 4):
            x = x + velocity_part
        elif f == 1 + d:
            x = x + pressure_part
        out.append(weight * x)
    return out


def axis_parity(axis):
    return lax.rem(lax.axis_index(axis), 2)


def one_hot(index_row, count):
    short = jnp.broadcast_to(index_row, (16, index_row.shape[1])).astype(jnp.int16)
    rows = lax.broadcasted_iota(jnp.int16, (16, index_row.shape[1]), 0)
    one, zero = jnp.ones(short.shape, BF), jnp.zeros(short.shape, BF)
    return jnp.concatenate([jnp.where(rows == short - r, one, zero) for r in range(0, count, 16)], 0)


def store_halves(ref_hi, ref_lo, at, cols, value):
    hi, lo = halves(jnp.concatenate([value, jnp.zeros((PAD - FACE, value.shape[1]), F32)], 0))
    ref_hi[at : at + PAD, cols] = hi
    ref_lo[at : at + PAD, cols] = lo


def turned(packed, code, turn_t, stack_hi, stack_lo):
    hi = packed.astype(BF).astype(F32)
    lo = packed - hi
    for c in range(8):
        stack_hi[c * PAD : (c + 1) * PAD, :] = jnp.where(code == c, hi, 0.0).astype(BF)
        stack_lo[c * PAD : (c + 1) * PAD, :] = jnp.where(code == c, lo, 0.0).astype(BF)
    return dot(turn_t[...], stack_hi[...]) + dot(turn_t[...], stack_lo[...])


def tile_cols(t):
    return slice(t * LANES, (t + 1) * LANES)


def neighbour_index(rows, slot_v):
    elems = slot_v.shape[1]
    own = one_hot(slot_v[...], elems)
    base = 256.0
    table = jnp.concatenate(rows + [jnp.zeros((8 - len(rows), elems), F32)], 0)
    upper = jnp.floor(table * (1.0 / base))
    lower = table - upper * base
    both = jnp.concatenate([upper, lower], 0).astype(BF)
    moved = dot_t(both, own)
    return (moved[0:8] * base + moved[8:16]).astype(jnp.int32)


def first_kernel(
    per_span, axial, sectors, slot_l, turn_l, offset_l, slot_h, fields, velocity, sound, turn_h, forward_h,
    staged, theta, iface, slot_v, plan, own_packed, forward_t, turn_t, rows_hi, rows_lo, stack_hi, stack_lo, slot_s, turn_s, offset_s,
    sems, small_sems,
):
    elems = slot_v.shape[1]
    tiles = elems // LANES
    half = axial // 2
    rows = VALS * PAD
    small = [
        pltpu.make_async_copy(slot_h, slot_v, small_sems.at[0]),
        pltpu.make_async_copy(turn_h, turn_t, small_sems.at[1]),
        pltpu.make_async_copy(slot_l, slot_s, small_sems.at[2]),
        pltpu.make_async_copy(turn_l, turn_s, small_sems.at[3]),
        pltpu.make_async_copy(offset_l, offset_s, small_sems.at[4]),
        pltpu.make_async_copy(forward_h, forward_t, small_sems.at[5]),
    ]
    loads = []
    for t in range(tiles):
        cols = pl.ds(t * LANES, LANES)
        loads.append([
            pltpu.make_async_copy(fields.at[:, :, cols], staged.at[0:5, t, 0:VOL, :], sems.at[t, 0]),
            pltpu.make_async_copy(velocity.at[:, :, cols], staged.at[5:8, t, 0:VOL, :], sems.at[t, 1]),
            pltpu.make_async_copy(sound.at[:, cols], staged.at[8, t, 0:VOL, :], sems.at[t, 2]),
        ])
        for copy in loads[-1]:
            copy.start()
    for copy in small:
        copy.start()
    for copy in small:
        copy.wait()
    sector = lax.axis_index("blk")
    lane = lane_iota((1, LANES))
    column = lane % (2 * per_span)
    target = jnp.full((1, LANES), -1, jnp.int32)
    code = jnp.zeros((1, LANES), jnp.int32)
    want = jnp.zeros((1, LANES), jnp.int32)
    forward = jnp.zeros((1, LANES), jnp.int32)
    for s in range(per_span):
        target = jnp.where(lane == s, slot_s[s * axial + half - 1], target)
        target = jnp.where(lane == per_span + s, slot_s[s * axial + half], target)
        code = jnp.where(column == per_span + s, turn_s[0, s], code)
        forward = jnp.where(column == s, turn_s[0, s], forward)
        shift = lax.rem(offset_s[s], sectors)
        want = jnp.where(column == s, lax.rem(sector - shift + sectors, sectors), want)
        want = jnp.where(column == per_span + s, lax.rem(sector + shift, sectors), want)
    plan[0:1, :] = want
    plan[1:2, :] = forward
    one = one_hot(target, elems)
    theta[VALS * FACE : VALS * FACE + 1, :] = jnp.zeros((1, elems), F32)
    odd = axis_parity("blk")

    for t in range(tiles):
        for copy in loads[t]:
            copy.wait()
        cols = tile_cols(t)

        @pl.when(odd == 0)
        def _():
            for f in range(VALS):
                theta[f * FACE : (f + 1) * FACE, cols] = face_rows(staged, value_index(f, 0), t, 0, ORDER)

        @pl.when(odd == 1)
        def _():
            for f in range(VALS):
                theta[f * FACE : (f + 1) * FACE, cols] = face_rows(staged, value_index(f, 0), t, 0, 0)

        for n, end in enumerate((ORDER, 0)):
            for f in range(VALS):
                at = n * rows + f * PAD
                store_halves(rows_hi, rows_lo, at, cols, face_rows(staged, value_index(f, 2), t, 2, end))
    both = dot(rows_hi[...], one) + dot(rows_lo[...], one)
    both = jnp.where(lane < per_span, both[0:rows], jnp.where(lane < 2 * per_span, both[rows:], 0.0))
    packed = both[0:PAD]
    for f in range(1, VALS):
        packed = packed + pltpu.roll(both[f * PAD : (f + 1) * PAD], f * 2 * per_span, 1)
    own_packed[...] = packed
    iface[...] = turned(packed, code, turn_t, stack_hi, stack_lo)
    for t in range(tiles):
        iface[PAD - tiles + t : PAD - tiles + t + 1, :] = slot_v[:, tile_cols(t)].astype(F32)


LOCAL_FACES = ((1, 1), (1, 0), (2, 1), (2, 0))


def second_kernel(
    per_span, axial, slot_v, staged, matrix_h, theta, sp_a, sp_b, index, rows_hi, rows_lo, matrix, sem,
):
    load = pltpu.make_async_copy(matrix_h, matrix, sem)
    load.start()
    elems = slot_v.shape[1]
    tiles = elems // LANES
    half = axial // 2
    rows = VALS * PAD
    theta[VALS * FACE : VALS * FACE + 1, :] = jnp.zeros((1, elems), F32)
    odd = axis_parity("blk")

    @pl.when(odd == 0)
    def _():
        for t in range(tiles):
            for f in range(VALS):
                theta[f * FACE : (f + 1) * FACE, tile_cols(t)] = face_rows(staged, value_index(f, 0), t, 0, 0)

    @pl.when(odd == 1)
    def _():
        for t in range(tiles):
            for f in range(VALS):
                theta[f * FACE : (f + 1) * FACE, tile_cols(t)] = face_rows(staged, value_index(f, 0), t, 0, ORDER)

    for n, (d, end) in enumerate(LOCAL_FACES):
        for t in range(tiles):
            for f in range(VALS):
                x = face_rows(staged, value_index(f, d), t, d, end * ORDER)
                store_halves(rows_hi, rows_lo, n * rows + f * PAD, tile_cols(t), x)

    def gathered(start, row):
        one = one_hot(row, elems)
        return dot(rows_hi[start : start + rows, :], one) + dot(rows_lo[start : start + rows, :], one)

    high = gathered(0, slot_v[:, elems - axial : elems])
    low = gathered(rows, slot_v[:, 0:axial])
    span_odd = axis_parity("span")

    @pl.when(span_odd == 0)
    def _():
        sp_a[...] = high
        sp_b[...] = low

    @pl.when(span_odd == 1)
    def _():
        sp_a[...] = low
        sp_b[...] = high

    slots = slot_v[...].astype(F32)
    lane = lane_iota((1, elems))
    position = lane % axial
    row = (lane // axial).astype(F32)
    lanes_f = lane.astype(F32)
    span_low = jnp.where(lane < axial, elems + lanes_f, pltpu.roll(slots, axial, 1))
    span_high = jnp.where(lane >= elems - axial, axial + lanes_f, pltpu.roll(slots, elems - axial, 1))
    none = elems + LANES - 1.0
    ax_low = jnp.where(position == half, elems + row, pltpu.roll(slots, 1, 1))
    ax_low = jnp.where(position == 0, none, ax_low)
    ax_high = jnp.where(position == half - 1, elems + per_span + row, pltpu.roll(slots, elems - 1, 1))
    ax_high = jnp.where(position == axial - 1, none, ax_high)
    index[...] = neighbour_index([span_low, span_high, ax_low, ax_high], slot_v)
    load.wait()


def local_kernel(index, rows_hi, rows_lo, ghosts):
    elems = index.shape[1]
    rows = VALS * PAD
    for n in range(len(LOCAL_FACES)):
        one = one_hot(index[n : n + 1, :], elems)
        at = slice(n * rows, (n + 1) * rows)
        ghosts[n] = dot(rows_hi[at, :], one) + dot(rows_lo[at, :], one)


def work_kernel(place, per_span, staged, index, ghosts, matrix, store_h, earlier, out, store, sems, *scratch):
    del earlier

    @pl.when(work_place() == place)
    def _():
        tiles = staged.shape[1]
        elems = tiles * LANES
        stores = [
            pltpu.make_async_copy(store_h.at[:, :, pl.ds(t * LANES, LANES)], store.at[:, t, 0:VOL, :], sems.at[t])
            for t in range(tiles)
        ]
        for copy in stores:
            copy.start()
        volume_terms(staged, matrix, out, *scratch)
        for copy in stores:
            copy.wait()
        for t in range(tiles):
            for f in range(5):
                out[f, t, 0:VOL, :] += section_decay * store[f, t, 0:VOL, :]
            for n, side in ((2, -1), (3, 1)):
                at = index[n : n + 1, tile_cols(t)]
                keep = jnp.logical_or(at < elems, at >= elems + 2 * per_span)
                side_terms(staged, ghosts.at[n], out, 2, side, t, keep=keep)


def work_start(place, per_span, staged, index, ghosts, matrix, store_h, out, *scratch):
    work_kernel(place, per_span, staged, index, ghosts, matrix, store_h, None, out, *scratch)


def work_place():
    return jnp.where(axis_parity("span") == 1, 0, 1)


def volume_terms(staged, matrix, out, flux_hi, flux_lo):
    tiles = staged.shape[1]
    step = 16
    for pair in range(tiles // 2):
        for half in range(2):
            t = 2 * pair + half
            cols = tile_cols(half)
            for r in range(0, VOL, step):
                n = min(step, VOL - r)
                rows = slice(r, r + n)
                q = [staged[f, t, rows, :] for f in range(5)]
                c = staged[8, t, rows, :]
                cp = c * q[4]
                for d in range(3):
                    m = staged[5 + d, t, rows, :]
                    cu = c * q[1 + d]
                    for f in range(5):
                        x = m * q[f]
                        if f in (0, 4):
                            x = x + cu
                        elif f == 1 + d:
                            x = x + cp
                        if n < step:
                            x = jnp.concatenate([x, jnp.zeros((step - n, LANES), F32)], 0)
                        hi, lo = halves(x)
                        flux_hi[pair, f, d * LANES + r : d * LANES + r + step, cols] = hi
                        flux_lo[pair, f, d * LANES + r : d * LANES + r + step, cols] = lo
        for f in range(5):
            a = dot(matrix[...], flux_hi[pair, f])
            b = dot(matrix[0:LANES, :], flux_lo[pair, f])
            total = a[0:LANES] + a[LANES : 2 * LANES] + b
            for half in range(2):
                out[f, 2 * pair + half] = total[:, tile_cols(half)]


def theta_ghost(recv, index_row):
    one = one_hot(index_row, recv.shape[1])
    hi, lo = halves(recv[...])
    return dot(hi, one) + dot(lo, one)


def theta_side(staged, ghost, acc, side, t):
    start = ORDER * FACE if side > 0 else 0
    own = [staged[value_index(f, 0), t, start : start + FACE, :] for f in range(VALS)]
    other = [ghost[f * FACE : (f + 1) * FACE, tile_cols(t)] for f in range(VALS)]
    for f, x in enumerate(surface(own, other, 0, side)):
        acc[f, t, start : start + FACE, :] += x


def side_terms(staged, ghost_ref, acc, d, side, t, keep=None, wall=None):
    cols = tile_cols(t)
    end = ORDER if side > 0 else 0
    own = [face_rows(staged, value_index(f, d), t, d, end) for f in range(VALS)]
    other = [ghost_ref[f * PAD : f * PAD + FACE, cols] for f in range(VALS)]
    if wall is not None:
        for f in range(VALS):
            other[f] = jnp.where(wall, -own[f] if f == 1 + d else own[f], other[f])
    for f, x in enumerate(surface(own, other, d, side)):
        add_face_rows(acc, f, t, d, end, x if keep is None else jnp.where(keep, x, 0.0))


def face_kernel(slot_v, staged, index, ghosts, th_a, sp_a, iface_a, part, acc, whole, ghost):
    del part
    tiles = staged.shape[1]
    odd = axis_parity("blk")
    slots_a = jnp.concatenate([iface_a[PAD - tiles + t : PAD - tiles + t + 1, :] for t in range(tiles)], 1)
    ghost[...] = theta_ghost(th_a, neighbour_index([slots_a], slot_v)[0:1])
    span_side(0, staged, index, ghosts, sp_a, acc, whole, None)
    for t in range(tiles):
        @pl.when(odd == 0)
        def _():
            theta_side(staged, ghost, acc, 1, t)

        @pl.when(odd == 1)
        def _():
            theta_side(staged, ghost, acc, -1, t)


def interface_kernel(
    per_span, sectors, pieces, far,
    plan, slot_v, index, own_packed, turn_t, part, *rest,
):
    del part
    iface = rest[:pieces]
    acc, picks, stack_hi, stack_lo = rest[pieces:]
    elems = slot_v.shape[1]
    tiles = elems // LANES
    sector = lax.axis_index("blk")
    odd = lax.rem(sector, 2)

    partner = lax.rem(sector + jnp.where(odd == 1, 1, sectors - 1), sectors)
    slots_b = jnp.zeros((tiles, LANES), F32)
    want, code = plan[0:1, :], plan[1:2, :]
    near = jnp.zeros((PAD, LANES), F32)
    blocks = [piece[b * PAD : (b + 1) * PAD, :] for piece in iface for b in range(piece.shape[0] // PAD)]
    for k, block in zip(far, blocks):
        near = jnp.where(want == (sector ^ k), block, near)
        slots_b = jnp.where(partner == (sector ^ k), block[PAD - tiles :], slots_b)
    flat = lambda x: jnp.concatenate([x[t : t + 1] for t in range(tiles)], 1)
    picks[...] = one_hot(neighbour_index([flat(slots_b)], slot_v)[0:1], elems)

    near = turned(near, code, turn_t, stack_hi, stack_lo)
    lane = lane_iota((1, LANES))
    used = lane < 2 * per_span
    own, other = [], []
    for f in range(VALS):
        at = f * 2 * per_span
        down = pltpu.roll(own_packed[...], LANES - at - per_span, 1)
        up = pltpu.roll(own_packed[...], (LANES - at + per_span) % LANES, 1)
        own.append(jnp.where(used, jnp.where(lane < per_span, down, up), 0.0))
        theirs = near if f == 0 else pltpu.roll(near, LANES - at, 1)
        other.append(jnp.where(used, theirs, 0.0))
    low = surface(own, other, 2, -1)
    high = surface(own, other, 2, 1)
    terms = jnp.concatenate([jnp.where(lane < per_span, x, y) for x, y in zip(low, high)], 0)
    hi, lo = halves(jnp.where(used, terms, 0.0))

    def placed(n):
        one = one_hot(index[n : n + 1, :] - elems, LANES)
        return dot(hi, one) + dot(lo, one)

    fixes = (placed(2), placed(3))

    for t in range(tiles):
        for f in range(5):
            for fix, end in zip(fixes, (0, ORDER)):
                add_face_rows(acc, f, t, 2, end, fix[f * PAD : f * PAD + FACE, tile_cols(t)])


def span_side(other_pair, staged, index, ghosts, received, acc, whole, wall, tile=None):
    slab_odd = axis_parity("span")
    for n, side in ((0, -1), (1, 1)):
        @pl.when(slab_odd == (1 - n if other_pair == 0 else n))
        def _():
            elems = index.shape[1]
            if tile in (None, 0):
                hi, lo = halves(received[...])
                one = one_hot(index[n : n + 1, :] - elems, LANES)
                whole[...] = ghosts[n] + (dot(hi, one) + dot(lo, one))
            for t in range(staged.shape[1]) if tile is None else (tile,):
                at_wall = None
                if wall is not None:
                    at_wall = jnp.logical_and(index[n : n + 1, tile_cols(t)] >= elems, wall)
                side_terms(staged, whole, acc, 1, side, t, wall=at_wall)


def late_kernel(slabs, staged, index, ghosts, sp_b, part, acc, whole):
    del part
    slab = lax.axis_index("span")
    span_side(1, staged, index, ghosts, sp_b, acc, whole, jnp.logical_or(slab == 0, slab == slabs - 1))


HIGH_ROW = (ORDER * FACE) // PAD * PAD
LOWER, MIDDLE, UPPER = slice(0, PAD), slice(PAD, HIGH_ROW), slice(HIGH_ROW, VOL)


def last_kernel(staged, picks, th_b, part, fields_out, store_out, acc, fresh, ghost, sems):
    del part
    tiles = staged.shape[1]
    odd = axis_parity("blk")
    copies = []

    def send(n, t, rows):
        for f in range(5):
            fresh[f, t, rows, :] = staged[f, t, rows, :] + section_gain * acc[f, t, rows, :]
        cols = pl.ds(t * LANES, LANES)
        pair = [
            pltpu.make_async_copy(acc.at[:, t, rows, :], store_out.at[:, rows, cols], sems.at[n, t, 0]),
            pltpu.make_async_copy(fresh.at[:, t, rows, :], fields_out.at[:, rows, cols], sems.at[n, t, 1]),
        ]
        for copy in pair:
            copy.start()
        copies.extend(pair)

    for t in range(tiles):
        send(0, t, MIDDLE)
    hi, lo = halves(th_b[...])
    ghost[...] = dot(hi, picks[...]) + dot(lo, picks[...])
    for t in range(tiles):
        @pl.when(odd == 0)
        def _():
            theta_side(staged, ghost, acc, -1, t)

        @pl.when(odd == 1)
        def _():
            theta_side(staged, ghost, acc, 1, t)

        send(1, t, LOWER)
        send(2, t, UPPER)
    for copy in copies:
        copy.wait()


def params(limit=VMEM_LIMIT):
    return pltpu.CompilerParams(vmem_limit_bytes=limit)


def vmem_spec():
    return pl.BlockSpec(memory_space=pltpu.VMEM)


def hbm_spec():
    return pl.BlockSpec(memory_space=pltpu.HBM)


def in_hbm(x):
    return pltpu.with_memory_space_constraint(x, pltpu.HBM)


def in_vmem(x):
    return pltpu.with_memory_space_constraint(x, pltpu.VMEM)


def reaches(sectors):
    steps = [1 << bit for bit in range(sectors.bit_length() - 1)]
    return steps[:1] + steps[:0:-1]


def on_device(fields, section_store, mean_velocity, sound_speed, element_slot, face_turn, rotor_offset):
    per_theta, per_span = face_turn.shape
    elems = element_slot.shape[0]
    axial = elems // (per_theta * per_span)
    sectors, slabs = lax.axis_size("blk"), lax.axis_size("span")
    tiles = elems // LANES
    rows = VALS * PAD
    assert per_theta == 1 and axial == LANES and sectors % 2 == 0 and sectors & (sectors - 1) == 0
    assert 2 * per_span * VALS < LANES and FACE + tiles <= PAD
    dma = pltpu.SemaphoreType.DMA
    theta_rows = VALS * FACE + 1
    vmem, hbm = pltpu.VMEM, pltpu.HBM
    slot_h = in_hbm(element_slot.reshape(1, elems))
    stack = [vmem((8 * PAD, LANES), BF), vmem((8 * PAD, LANES), BF)]
    staged, th_a, iface, slot_v, plan, own_packed, forward_t = pl.pallas_call(
        functools.partial(first_kernel, per_span, axial, sectors),
        out_shape=(
            vmem((9, tiles, LANES, LANES), F32),
            vmem((theta_rows, elems), F32),
            vmem((PAD, LANES), F32),
            vmem((1, elems), jnp.int32),
            vmem((8, LANES), jnp.int32),
            vmem((PAD, LANES), F32),
            vmem((PAD, 8 * PAD), BF),
        ),
        in_specs=[hbm_spec()] * 9,
        out_specs=(vmem_spec(),) * 7,
        scratch_shapes=[
            vmem((PAD, 8 * PAD), BF),
            vmem((2 * rows, elems), BF),
            vmem((2 * rows, elems), BF),
            *stack,
            pltpu.SMEM((elems,), jnp.int32),
            pltpu.SMEM((per_theta, per_span), jnp.int32),
            pltpu.SMEM((per_span,), jnp.int32),
            dma((tiles, 3)),
            dma((6,)),
        ],
        compiler_params=params(),
        name="first",
    )(
        in_hbm(element_slot), in_hbm(face_turn), in_hbm(rotor_offset), slot_h, in_hbm(fields), in_hbm(mean_velocity), in_hbm(sound_speed),
        in_hbm(jnp.asarray(turn_matrix(True))), in_hbm(jnp.asarray(turn_matrix(False))),
    )

    pieces, far = [iface], [0]
    near_a = lax.ppermute(th_a, "blk", [(i, i ^ 1) for i in range(sectors)])
    for reach in reaches(sectors):
        block = jnp.concatenate(pieces, 0)
        pieces.append(lax.ppermute(block, "blk", [(i, i ^ reach) for i in range(sectors)]))
        far += [k ^ reach for k in far]

    th_b, sp_a, sp_b, index, rows_hi, rows_lo, matrix = pl.pallas_call(
        functools.partial(second_kernel, per_span, axial),
        out_shape=(
            vmem((theta_rows, elems), F32),
            vmem((rows, LANES), F32),
            vmem((rows, LANES), F32),
            vmem((8, elems), jnp.int32),
            vmem((len(LOCAL_FACES) * rows, elems), BF),
            vmem((len(LOCAL_FACES) * rows, elems), BF),
            vmem((2 * LANES, 3 * LANES), BF),
        ),
        in_specs=[vmem_spec()] * 2 + [hbm_spec()],
        out_specs=(vmem_spec(),) * 7,
        scratch_shapes=[dma(())],
        compiler_params=params(),
        name="second",
    )(in_vmem(slot_v), in_vmem(staged), in_hbm(jnp.asarray(volume_matrix())))
    pairs = [(i, (i + 1 if i % 2 else i - 1) % sectors) for i in range(sectors)]
    near_b = lax.ppermute(th_b, "blk", pairs)
    span_a = lax.ppermute(sp_a, "span", [(i, i ^ 1) for i in range(slabs) if i ^ 1 < slabs])
    pairs = [(i, i + 1 if i % 2 else i - 1) for i in range(slabs)]
    span_b = lax.ppermute(sp_b, "span", [(i, j) for i, j in pairs if 0 <= j < slabs])

    ghosts = pl.pallas_call(
        local_kernel,
        out_shape=vmem((len(LOCAL_FACES), rows, elems), F32),
        in_specs=[vmem_spec()] * 3,
        out_specs=vmem_spec(),
        compiler_params=params(),
        name="local",
    )(in_vmem(index), in_vmem(rows_hi), in_vmem(rows_lo))

    part = None
    block = (5, tiles, LANES, LANES)
    for place in range(2):
        work = pl.pallas_call(
            functools.partial(work_kernel if place else work_start, place, per_span),
            out_shape=vmem(block, F32),
            in_specs=[vmem_spec()] * 4 + [hbm_spec()] + [vmem_spec()] * (place > 0),
            out_specs=vmem_spec(),
            scratch_shapes=[
                vmem(block, F32),
                dma((tiles,)),
                vmem((tiles // 2, 5, 3 * LANES, 2 * LANES), BF),
                vmem((tiles // 2, 5, 3 * LANES, 2 * LANES), BF),
            ],
            input_output_aliases={5: 0} if place else {},
            compiler_params=params(),
        )
        operands = [in_vmem(staged), in_vmem(index), in_vmem(ghosts)]
        operands += [in_vmem(matrix), in_hbm(section_store)]
        if place:
            operands.append(in_vmem(part))
        part = work(*operands)

    part = pl.pallas_call(
        face_kernel,
        out_shape=vmem(block, F32),
        in_specs=[vmem_spec()] * 8,
        out_specs=vmem_spec(),
        scratch_shapes=[vmem((rows, elems), F32), vmem((theta_rows, elems), F32)],
        input_output_aliases={7: 0},
        compiler_params=params(),
        name="faces",
    )(
        in_vmem(slot_v), in_vmem(staged), in_vmem(index), in_vmem(ghosts), in_vmem(near_a), in_vmem(span_a),
        in_vmem(pieces[1]), in_vmem(part),
    )

    part, picks = pl.pallas_call(
        functools.partial(interface_kernel, per_span, sectors, len(pieces), far),
        out_shape=(vmem(block, F32), vmem((elems, elems), BF)),
        in_specs=[vmem_spec()] * (6 + len(pieces)),
        out_specs=(vmem_spec(),) * 2,
        scratch_shapes=stack,
        input_output_aliases={5: 0},
        compiler_params=params(),
        name="interface",
    )(
        in_vmem(plan), in_vmem(slot_v), in_vmem(index), in_vmem(own_packed), in_vmem(forward_t), in_vmem(part),
        *[in_vmem(piece) for piece in pieces],
    )

    part = pl.pallas_call(
        functools.partial(late_kernel, slabs),
        out_shape=vmem(block, F32),
        in_specs=[vmem_spec()] * 5,
        out_specs=vmem_spec(),
        scratch_shapes=[vmem((rows, elems), F32)],
        input_output_aliases={4: 0},
        compiler_params=params(),
        name="late",
    )(in_vmem(staged), in_vmem(index), in_vmem(ghosts), in_vmem(span_b), in_vmem(part))

    whole = hbm((5, VOL, elems), F32)
    fields_next, store_next, _ = pl.pallas_call(
        last_kernel,
        out_shape=(whole, whole, vmem(block, F32)),
        in_specs=[vmem_spec()] * 4,
        out_specs=(hbm_spec(),) * 2 + (vmem_spec(),),
        scratch_shapes=[vmem(block, F32), vmem((theta_rows, elems), F32), dma((3, tiles, 2))],
        input_output_aliases={3: 2},
        compiler_params=params(),
        name="last",
    )(in_vmem(staged), in_vmem(picks), in_vmem(near_b), in_vmem(part))
    return fields_next, store_next


def solution(mesh):
    both = ("blk", "span")
    in_specs = (
        P(None, None, both),
        P(None, None, both),
        P(None, None, both),
        P(None, both),
        P(both),
        P("blk", "span"),
        P("span"),
    )
    out_specs = (P(None, None, both), P(None, None, both))
    return jax.shard_map(on_device, mesh=mesh, in_specs=in_specs, out_specs=out_specs, check_vma=False)
```
